128 devices in a mesh: gx: 32 (over x, y, core), gy: 4 (over z).
Axes of the slice: x: 4, y: 4, z: 4, core: 2. Of those that a mesh axis runs over, the one named last changes fastest.
Arguments:
- signals: float32 [64, 32, 16, 128], P('gx', 'gy'), may hold values from -6 to 6
- tiles: bfloat16 [64, 32, 4, 128, 128], P('gx', 'gy'), may hold values from 0 to 0.00390625
- tile_dir: int32 [64, 32, 4], P('gx', 'gy'), may hold values from 0 to 8
- tile_mask: int32 [64, 32, 4], P('gx', 'gy'), may hold values 0 or 1
- live_rows: int32 [64, 32], P('gx', 'gy'), may hold values from 32 to 128
- bound_rows: int32 [64, 32], P('gx', 'gy'), may hold values from 1 to 32, as said below
- scale_coeffs: float32 [6, 5], replicated, may hold values from -1 to 1
- spectral_bound: float32 [1], replicated, may hold values from 2.5 to 4
Outputs:
- coefficients: float32 [6, 64, 32, 16, 128], P(None, 'gx', 'gy')
- energy: float32 [6, 16], replicated
The draws below stay inside these ranges and needn't reach their ends.
Inputs may be any that keep to these rules, and one draw needn't show every extreme that they name: `bound_rows`: in every draw, some blocks on every device have exactly 32 boundary rows.
All inputs are finite; a program needn't handle non-finite values. No bound on the sum of `tile_mask` on one device may be relied on, other than what follows from the above.
Results may differ from the reference program's by a relative error of at most 0.0003.
Values may be sent and summed in bfloat16 or wider, within the bound.
A program may use at most 64 MiB of HBM per device.

```python
import jax
import jax.numpy as jnp
from jax import lax

SIG = 16
SCALES = 6
DEG = 4
SLOTS = 4
TILE = 128
BMAX = 32
BY = 8
NBX = 64
NBY = 32


def draw_bound_rows(key, part):
    drawn = jax.random.randint(key, (NBX, NBY), 1, BMAX + 1, dtype=jnp.int32)
    columns = lax.broadcasted_iota(jnp.int32, (NBX, NBY), 1)
    return jnp.where(columns % BY == 0, jnp.int32(BMAX), drawn)


def with_ends(values, own_key, low, high):
    spot = [jax.random.randint(jax.random.fold_in(own_key, axis), (), 0, length) for axis, length in enumerate(values.shape)]
    main_axis = values.shape.index(max(values.shape))
    next_to = spot[:main_axis] + [(spot[main_axis] + 1) % values.shape[main_axis]] + spot[main_axis + 1:]
    return values.at[tuple(spot)].set(low).at[tuple(next_to)].set(high)


def steps_of(key, shape, cuts, low, high):
    def one(position, shards_of):
        steps = jax.random.uniform(jax.random.fold_in(jax.random.fold_in(key, 6), position), (shards_of,), jnp.float32, low / len(cuts), high / len(cuts))
        return jnp.repeat(jnp.exp(steps), shape[position] // shards_of).reshape((-1,) + (1,) * (len(shape) - position - 1))

    factor_of = one(*cuts[0])
    for cut in cuts[1:]:
        factor_of = factor_of * one(*cut)
    return factor_of


def scatter_about(key, dims, spread, limit, cuts=(), held_as=jnp.bfloat16):
    values = jax.random.normal(key, dims, jnp.float32) * spread
    if len(cuts) > 0:
        values = steps_of(key, dims, cuts, -0.22, 0.18) * values
    return jnp.clip(values, min=-limit, max=limit).astype(held_as)


def setup_inputs(seed: int = 0) -> dict:
    key_list = jax.random.split(jax.random.key(seed), 9)
    return {
        "signals": scatter_about(key_list[0], (NBX, NBY, SIG, TILE), 1.0, 6.0, ((0, 32), (1, 4)), jnp.float32),
        "tiles": jnp.clip(0.00390625 * jax.random.uniform(key_list[1], (NBX, NBY, SLOTS, TILE, TILE), jnp.float32) ** steps_of(key_list[1], (NBX, NBY, SLOTS, TILE, TILE), ((0, 32), (1, 4)), -0.2, 0.2), 0.0, 0.00390625).astype(jnp.bfloat16),
        "tile_dir": with_ends(jax.random.randint(key_list[2], (NBX, NBY, SLOTS), 0, 9), jax.random.fold_in(key_list[2], 1), 0, 8).astype(jnp.int32),
        "tile_mask": with_ends((jax.random.randint(key_list[3], (NBX, NBY, SLOTS), 0, 4) < 3).astype(jnp.int32), jax.random.fold_in(key_list[3], 1), 0, 1),
        "live_rows": with_ends(jax.random.randint(key_list[4], (NBX, NBY), TILE // 4, TILE + 1), jax.random.fold_in(key_list[4], 1), TILE // 4, TILE).astype(jnp.int32),
        "bound_rows": draw_bound_rows(jax.random.fold_in(key_list[8], 71), 0),
        "scale_coeffs": jnp.clip(jax.random.uniform(key_list[6], (SCALES, DEG + 1), jnp.float32, -1.0, 1.0), -1.0, 1.0),
        "spectral_bound": jnp.clip(jax.random.uniform(key_list[7], (1,), jnp.float32, 2.5, 4.0), 2.5, 4.0),
    }


def adjacency(values, tiles, tile_dir, tile_mask, bound_ind):
    own_rows = values.astype(jnp.bfloat16)
    edge_rows = (values * bound_ind[:, :, None, :]).astype(jnp.bfloat16)
    padded = jnp.pad(edge_rows, ((1, 1), (1, 1), (0, 0), (0, 0)))
    extent_x = values.shape[0]
    extent_y = values.shape[1]
    slot_list = []
    for slot_index in range(SLOTS):
        picked = jnp.zeros_like(own_rows)
        for direction in range(9):
            step_x = direction // 3 - 1
            step_y = direction % 3 - 1
            if direction == 4:
                source = own_rows
            else:
                source = padded[1 + step_x:1 + step_x + extent_x, 1 + step_y:1 + step_y + extent_y]
            matches = (tile_dir[:, :, slot_index] == direction)[:, :, None, None]
            picked = jnp.where(matches, source, picked)
        kept_mask = (tile_mask[:, :, slot_index] == 1)[:, :, None, None]
        picked = jnp.where(kept_mask, picked, jnp.zeros_like(picked))
        slot_list.append(picked)
    inputs = jnp.stack(slot_list, axis=2)

    def one_row(bundle):
        tile_row, input_row = bundle
        return jnp.einsum("jsrc,jsgc->jgr", tile_row.astype(jnp.float32), input_row.astype(jnp.float32))

    return lax.map(one_row, (tiles, inputs))


def scaled_laplacian(values, adjacent, degree, factor):
    return factor * (degree * values - adjacent) - values


def reference(signals, tiles, tile_dir, tile_mask, live_rows, bound_rows, scale_coeffs, spectral_bound):
    positions = lax.broadcasted_iota(jnp.int32, (1, 1, TILE), 2)
    live_ind = (positions < live_rows[:, :, None]).astype(jnp.float32)
    bound_ind = (positions < bound_rows[:, :, None]).astype(jnp.float32)
    initial = signals * live_ind[:, :, None, :]
    joined = jnp.concatenate([initial, live_ind[:, :, None, :]], axis=2)
    first_pass = adjacency(joined, tiles, tile_dir, tile_mask, bound_ind) * live_ind[:, :, None, :]
    degree = first_pass[:, :, SIG:, :]
    factor = 2.0 / spectral_bound[0]
    previous = initial
    current = scaled_laplacian(initial, first_pass[:, :, :SIG, :], degree, factor)
    totals = 0.5 * scale_coeffs[:, 0][:, None, None, None, None] * initial[None]
    totals = totals + scale_coeffs[:, 1][:, None, None, None, None] * current[None]
    for degree_index in range(2, DEG + 1):
        adjacent = adjacency(current, tiles, tile_dir, tile_mask, bound_ind) * live_ind[:, :, None, :]
        following = 2.0 * scaled_laplacian(current, adjacent, degree, factor) - previous
        previous = current
        current = following
        totals = totals + scale_coeffs[:, degree_index][:, None, None, None, None] * current[None]
    energy = jnp.sum(totals * totals, axis=(1, 2, 4)) / (NBX * NBY * TILE)
    return totals, energy
```

```python
import functools

import jax
import jax.numpy as jnp
from jax import lax
from jax.experimental import pallas as pl
from jax.experimental.pallas import tpu as pltpu
from jax.sharding import PartitionSpec as P

DEG = 4
EDGE = 32
VMEM_LIMIT = 24 * 1024 * 1024
MESH = pl.DeviceIdType.MESH
NT = (((1,), (1,)), ((), ()))
SIDES = ((-1, 0), (1, 0), (0, -1), (0, 1), (-1, -1), (-1, 1), (1, -1), (1, 1))
X_BASE, Z_BASE, C_BASE, ZERO = 16, 32, 36, 40


def kernel(
    nx, ny, sig_hbm, tiles_hbm, tdir_hbm, tmask_hbm, live_hbm, edge_hbm, coef_hbm, bound,
    totals, en_in,
    sig, tdir, tmask, live_rows, bound_rows, coef, index, used, tiles, w_edge, own, acc,
    cheb, slope, scale, cells, x_out, x_in, z_in, c_in,
    in_sem, tile_sem, send_sem, recv_sem, en_sem,
):
    ex, ey, chan, size = sig.shape
    slots = tiles.shape[2]
    scales = coef.shape[0]
    groups = size // EDGE
    quads = ey // groups
    n = nx * ny
    bf, f32 = jnp.bfloat16, jnp.float32
    gx, gy = lax.axis_index("gx"), lax.axis_index("gy")
    me = gx * ny + gy
    corners = [(i, j) for j in (0, ey - 1) for i in range(ex)]
    inner = [(i, j) for j in range(1, ey - 1) for i in range(ex)]
    blocks = corners + inner

    fetches = [
        pltpu.make_async_copy(src, dst, in_sem.at[k])
        for k, (src, dst) in enumerate(
            [
                (sig_hbm, sig), (live_hbm, live_rows), (edge_hbm, bound_rows), (tdir_hbm, tdir),
                (tmask_hbm, tmask), (coef_hbm, coef),
            ]
        )
    ]
    for copy in fetches:
        copy.start()
    tile_groups = tile_sem.shape[0]
    span = ey // tile_groups

    def tile_copy(k):
        part = pl.ds(k * span, span)
        return pltpu.make_async_copy(tiles_hbm.at[:, part], tiles.at[:, part], tile_sem.at[k])

    for k in range(tile_groups):
        tile_copy(k).start()

    for r in range(DEG):
        for ref in (x_in[r], z_in[r], c_in[r]):
            ref[...] = jnp.zeros(ref.shape, ref.dtype)
    for k in range(len(cells)):
        cells[k][ZERO] = jnp.zeros(cells[k].shape[1:], bf)

    barrier = pltpu.get_barrier_semaphore()

    def others(act):
        def one(kx, px, ky):
            py = gy + ky
            act(kx * ny + ky, px, jnp.where(py >= ny, py - ny, py))

        for ky in range(1, ny):
            one(0, gx, ky)

        @pl.loop(1, nx)
        def _(kx):
            px = gx + kx
            px = jnp.where(px >= nx, px - nx, px)
            for ky in range(ny):
                one(kx, px, ky)

    def greet(k, px, py):
        pl.semaphore_signal(barrier, inc=1, device_id=(px, py), device_id_type=MESH)

    others(greet)

    def inside(dx, dy):
        ok = None
        for d, g, m in ((dx, gx, nx), (dy, gy, ny)):
            if d:
                here = g > 0 if d < 0 else g < m - 1
                ok = here if ok is None else jnp.logical_and(ok, here)
        return ok

    def flat(i, j):
        return j * ex + i

    for copy in fetches:
        copy.wait()

    lane = lax.broadcasted_iota(jnp.int32, (1, size), 1)
    factor = 2.0 / jnp.full((1, size), bound[0], f32)
    group = [
        jnp.logical_and(lane >= s * EDGE, lane < (s + 1) * EDGE).astype(bf) for s in range(groups)
    ]

    def live_of(i, j):
        return (lane < live_rows[i, j]).astype(f32)

    def spread(v, i, j):
        v = v * (lane < bound_rows[i, j]).astype(f32)
        step = EDGE
        while step < size:
            v = v + pltpu.roll(v, step, 1)
            step *= 2
        return v.astype(bf)

    first_row = lax.broadcasted_iota(jnp.int32, (chan, size), 0) == 0

    def prepare(i, j):
        b = flat(i, j)
        live = live_of(i, j)
        v = sig[i, j] * live
        cheb[0, b] = v
        ind = jnp.where(first_row, jnp.broadcast_to(live, (chan, size)), 0.0)
        joined = jnp.concatenate([v, ind], axis=0)
        own[0][b] = joined.astype(bf)
        cells[0][b] = spread(joined, i, j)

    def message(r, k):
        dx, dy = SIDES[k]
        now = cells[min(r, 1 + (r + 1) % 2)]
        x = 0 if dx < 0 else 1
        y = 0 if dy < 0 else 1
        if dy == 0:
            src, dst = x_out[r].at[x], x_in[r].at[1 - x]
        elif dx == 0:
            src, dst = now.at[pl.ds(flat(0, y * (ey - 1)), ex)], z_in[r].at[1 - y]
        else:
            src = now.at[flat(x * (ex - 1), y * (ey - 1))]
            dst = c_in[r].at[2 * (1 - x) + 1 - y]
        return pltpu.make_async_remote_copy(
            src_ref=src,
            dst_ref=dst,
            send_sem=send_sem.at[k],
            recv_sem=recv_sem.at[r % 2, k],
            device_id=(gx + dx, gy + dy),
            device_id_type=MESH,
        )

    def each(chosen, act, sign):
        for k in chosen:
            dx, dy = SIDES[k]

            @pl.when(inside(sign * dx, sign * dy))
            def _():
                act(k)

    x_sides, z_sides, c_sides = (0, 1), (2, 3), (4, 5, 6, 7)

    def send(r, chosen):
        each(chosen, lambda k: message(r, k).start(), 1)

    def sent(r):
        each(c_sides + z_sides + x_sides, lambda k: message(r, k).wait_send(), 1)

    def receive(r, chosen):
        each(chosen, lambda k: message(r, k).wait_recv(), -1)

    def cells_of(r):
        return cells[min(r, 1 + (r + 1) % 2)]

    def pack(r):
        for side in range(2):
            i = side * (ex - 1)
            for q in range(quads):
                packed = None
                for t in range(groups):
                    term = cells_of(r)[flat(i, q * groups + t)] * group[t]
                    packed = term if packed is None else packed + term
                x_out[r][side, q] = packed

    def unpack_x(r):
        for side in range(2):
            for q in range(quads):
                v = x_in[r][side, q]
                at = X_BASE + (side * quads + q) * groups
                cells_of(r)[at] = v
                v = v.astype(f32)
                for t in range(1, groups):
                    cells_of(r)[at + t] = pltpu.roll(v, t * EDGE, 1).astype(bf)

    def unpack_zc(r):
        for y in range(2):
            for i in range(ex):
                cells_of(r)[Z_BASE + y * ex + i] = z_in[r][y, i]
        for k in range(4):
            cells_of(r)[C_BASE + k] = c_in[r][k]

    def tables(i, j):
        b = flat(i, j)
        for s in range(slots):
            d = tdir[i, s, j]
            live = tmask[i, s, j] == 1
            row = (d * 11) >> 5
            ti = row + (i - 1)
            tj = d - 3 * row + (j - 1)
            at = tj * ex + ti
            up, down = ti < 0, ti > ex - 1
            at_x = X_BASE + (tj >> 2) * groups + ((s - tj) & 3)
            at = jnp.where(up, at_x, jnp.where(down, at_x + quads * groups, at))
            if j in (0, ey - 1):
                y = 0 if j == 0 else 1
                out = tj < 0 if j == 0 else tj > ey - 1
                at_z = Z_BASE + y * ex + ti
                at_z = jnp.where(up, C_BASE + y, jnp.where(down, C_BASE + 2 + y, at_z))
                at = jnp.where(out, at_z, at)
            mine = jnp.logical_and(live, d == 4)
            index[b * slots + s] = jnp.where(jnp.logical_and(live, d != 4), at, ZERO)
            used[b * slots + s] = jnp.where(mine, 1.0, 0.0)

    def weights(i, j):
        packed = None
        for s in range(slots):
            tile = tiles[i, j, s].astype(f32)
            rolled = pltpu.roll(tile, s * EDGE, 1) if s else tile
            packed = rolled if packed is None else jnp.where(lane >= s * EDGE, rolled, packed)
        w_edge[flat(i, j)] = packed.astype(bf)

    def own_product(r, i, j):
        b = flat(i, j)
        mine = own[min(r, 1)][b]
        total = None
        for s in range(0, slots, 2):
            pair = jnp.concatenate(
                [mine * used[b * slots + s + k].astype(bf) for k in range(2)], axis=1
            )
            tile = jnp.concatenate([tiles[i, j, s + k] for k in range(2)], axis=1)
            term = lax.dot_general(pair, tile, NT, preferred_element_type=f32)
            total = term if total is None else total + term
        if r == 0:
            acc[b] = total
        else:
            acc[b, :chan] = 2.0 * (slope[b] * cheb[r, b] - scale[b] * total) - cheb[r - 1, b]

    def edge_product(r, i, j):
        b = flat(i, j)
        picked = None
        for s in range(slots):
            term = cells_of(r)[index[b * slots + s]] * group[s]
            picked = term if picked is None else picked + term
        return lax.dot_general(picked, w_edge[b], NT, preferred_element_type=f32)

    def add_totals(k):
        for s in range(scales):
            c = coef[s, k] * (0.5 if k == 0 else 1.0)
            for i, j in blocks:
                term = c * cheb[k, flat(i, j)]
                totals[s, i, j] = term if k == 0 else totals[s, i, j] + term

    sums = [None] * scales

    def advance(r, i, j):
        b = flat(i, j)
        edge = edge_product(r, i, j)
        if r == 0:
            adj = acc[b] + edge
            s = factor * live_of(i, j)
            m = s * adj[chan : chan + 1] - 1.0
            scale[b] = s
            slope[b] = m
            following = m * cheb[0, b] - s * adj[:chan]
        else:
            following = acc[b, :chan] - (2.0 * scale[b]) * edge
        cheb[r + 1, b] = following
        if r < DEG - 1:
            own[1][b] = following.astype(bf)
            cells_of(r + 1)[b] = spread(following, i, j)
        else:
            for s in range(scales):
                t = totals[s, i, j] + coef[s, DEG] * following
                sums[s] = t * t if sums[s] is None else sums[s] + t * t

    for i, j in corners:
        prepare(i, j)
    for i, j in inner:
        prepare(i, j)
    pack(0)
    pl.semaphore_wait(barrier, n - 1)
    send(0, c_sides)
    send(0, z_sides)
    send(0, x_sides)
    for i, j in blocks:
        tables(i, j)
    for r in range(DEG):
        if r == 0:
            for k in range(tile_groups):
                tile_copy(k).wait()
            for i, j in blocks:
                weights(i, j)
        for i, j in blocks:
            own_product(r, i, j)
        add_totals(r)
        sent(r)
        receive(r, x_sides)
        unpack_x(r)
        for i, j in inner:
            advance(r, i, j)
        receive(r, z_sides + c_sides)
        unpack_zc(r)
        for i, j in corners:
            advance(r, i, j)
        if r < DEG - 1:
            send(r + 1, c_sides)
            send(r + 1, z_sides)
            pack(r + 1)
            send(r + 1, x_sides)

    width = en_in.shape[2]
    if width > scales * chan:
        sums.append(jnp.zeros((width - scales * chan, size), f32))
    stacked = jnp.concatenate(sums, axis=0)
    high = stacked.astype(bf)
    low = (stacked - high.astype(f32)).astype(bf)
    local = lax.dot_general(
        jnp.ones((chan, 2 * size), bf), jnp.concatenate([high, low], axis=1), NT,
        preferred_element_type=f32,
    )
    en_in[me] = local[:1]

    def share(k, px, py):
        return pltpu.make_async_remote_copy(
            src_ref=en_in.at[me],
            dst_ref=en_in.at[me],
            send_sem=en_sem.at[0],
            recv_sem=en_sem.at[1],
            device_id=(px, py),
            device_id_type=MESH,
        )

    others(lambda k, px, py: share(k, px, py).start())

    for s in range(scales):
        c = coef[s, DEG]
        for i, j in blocks:
            totals[s, i, j] = totals[s, i, j] + c * cheb[DEG, flat(i, j)]

    rest = en_in.at[pl.ds(0, n - 1)]
    pltpu.make_async_copy(rest, rest, en_sem.at[1]).wait()
    pltpu.make_async_copy(rest, rest, en_sem.at[0]).wait()


def hand_out(count, made, shared, out_hbm, energy_out, energy, sem):
    scales, ex, ey, chan, size = made.shape
    stores = [
        pltpu.make_async_copy(made.at[s], out_hbm.at[s], sem.at[s]) for s in range(scales)
    ]
    for store in stores:
        store.start()
    total = jnp.sum(shared[...], axis=0) * (1.0 / count)
    for s in range(scales):
        energy[s : s + 1, :] = total[:, s * chan : (s + 1) * chan]
    stores.append(pltpu.make_async_copy(energy, energy_out, sem.at[scales]))
    stores[-1].start()
    for store in stores:
        store.wait()


def solution(mesh):
    nx, ny = mesh.shape["gx"], mesh.shape["gy"]
    n = nx * ny

    def shards(
        signals, tiles, tile_dir, tile_mask, live_rows, bound_rows, scale_coeffs, spectral_bound
    ):
        ex, ey, chan, size = signals.shape
        slots = tiles.shape[2]
        scales = scale_coeffs.shape[0]
        nb = ex * ey
        width = -(-scales * chan // 128) * 128
        quads = ey * EDGE // size
        bf, f32 = jnp.bfloat16, jnp.float32
        vmem = pl.BlockSpec(memory_space=pltpu.VMEM)
        hbm = pl.BlockSpec(memory_space=pltpu.HBM)
        rows = [chan * (2 if r == 0 else 1) for r in range(DEG)]
        made, shared = pl.pallas_call(
            functools.partial(kernel, nx, ny),
            out_shape=(
                jax.ShapeDtypeStruct((scales, ex, ey, chan, size), f32),
                jax.ShapeDtypeStruct((n, 1, width), f32),
            ),
            in_specs=[hbm] * 7 + [pl.BlockSpec(memory_space=pltpu.SMEM)],
            out_specs=(vmem, vmem),
            scratch_shapes=[
                pltpu.VMEM(signals.shape, f32),
                pltpu.SMEM((ex, slots, ey), jnp.int32),
                pltpu.SMEM((ex, slots, ey), jnp.int32),
                pltpu.SMEM((ex, ey), jnp.int32),
                pltpu.SMEM((ex, ey), jnp.int32),
                pltpu.SMEM(scale_coeffs.shape, f32),
                pltpu.SMEM((nb * slots,), jnp.int32),
                pltpu.SMEM((nb * slots,), f32),
                pltpu.VMEM((ex, ey, slots, size, size), bf),
                pltpu.VMEM((nb, size, size), bf),
                [pltpu.VMEM((nb, 2 * chan, size), bf), pltpu.VMEM((nb, chan, size), bf)],
                pltpu.VMEM((nb, 2 * chan, size), f32),
                pltpu.VMEM((DEG + 1, nb, chan, size), f32),
                pltpu.VMEM((nb, 1, size), f32),
                pltpu.VMEM((nb, 1, size), f32),
                [pltpu.VMEM((ZERO + 1, rows[min(k, 1)], size), bf) for k in range(3)],
                [pltpu.VMEM((2, quads, rows[r], size), bf) for r in range(DEG)],
                [pltpu.VMEM((2, quads, rows[r], size), bf) for r in range(DEG)],
                [pltpu.VMEM((2, ex, rows[r], size), bf) for r in range(DEG)],
                [pltpu.VMEM((4, rows[r], size), bf) for r in range(DEG)],
                pltpu.SemaphoreType.DMA((6,)),
                pltpu.SemaphoreType.DMA((4,)),
                pltpu.SemaphoreType.DMA((8,)),
                pltpu.SemaphoreType.DMA((2, 8)),
                pltpu.SemaphoreType.DMA((2,)),
            ],
            compiler_params=pltpu.CompilerParams(
                collective_id=0, has_side_effects=True, vmem_limit_bytes=VMEM_LIMIT
            ),
        )(
            *[
                pltpu.with_memory_space_constraint(a, pltpu.HBM)
                for a in (
                    signals, tiles, jnp.swapaxes(tile_dir, 1, 2), jnp.swapaxes(tile_mask, 1, 2),
                    live_rows, bound_rows, scale_coeffs,
                )
            ], spectral_bound
        )
        return pl.pallas_call(
            functools.partial(hand_out, n * nb * size),
            out_shape=(
                jax.ShapeDtypeStruct(made.shape, f32),
                jax.ShapeDtypeStruct((scales, chan), f32),
            ),
            in_specs=[vmem] * 2,
            out_specs=(hbm, hbm),
            scratch_shapes=[
                pltpu.VMEM((scales, chan), f32),
                pltpu.SemaphoreType.DMA((scales + 1,)),
            ],
            compiler_params=pltpu.CompilerParams(vmem_limit_bytes=VMEM_LIMIT),
        )(made, shared)

    placed = (
        P("gx", "gy", None, None),
        P("gx", "gy", None, None, None),
        P("gx", "gy", None),
        P("gx", "gy", None),
        P("gx", "gy"),
        P("gx", "gy"),
        P(),
        P(),
    )
    return jax.shard_map(
        shards,
        mesh=mesh,
        in_specs=placed,
        out_specs=(P(None, "gx", "gy", None, None), P()),
        check_vma=False,
    )
```

```python
import functools

import jax
import jax.numpy as jnp
from jax import lax
from jax.experimental import pallas as pl
from jax.experimental.pallas import tpu as pltpu
from jax.sharding import PartitionSpec as P

DEG = 4
EDGE = 32
VMEM_LIMIT = 24 * 1024 * 1024
MESH = pl.DeviceIdType.MESH
NT = (((1,), (1,)), ((), ()))
SIDES = ((-1, 0), (1, 0), (0, -1), (0, 1), (-1, -1), (-1, 1), (1, -1), (1, 1))
FAR = 4
JUMPS = ((-4, 4), (-8, 8), (16,))
X_BASE, Z_BASE, C_BASE, ZERO = 16, 32, 36, 40


def kernel(
    nx, ny, sig_hbm, tiles_hbm, tdir_hbm, tmask_hbm, live_hbm, edge_hbm, coef_hbm, bound,
    totals, en_in,
    sig, tdir, tmask, live_rows, bound_rows, coef, index, used, tiles, w_edge, own, acc,
    copies, cheb, slope, scale, cells, x_out, x_in, z_in, c_in,
    in_sem, tile_sem, send_sem, recv_sem, en_sem, know_sem,
):
    ex, ey, chan, size = sig.shape
    slots = tiles.shape[2]
    scales = coef.shape[0]
    groups = size // EDGE
    quads = ey // groups
    n = nx * ny
    bf, f32 = jnp.bfloat16, jnp.float32
    gx, gy = lax.axis_index("gx"), lax.axis_index("gy")
    me = gx * ny + gy
    corners = [(i, j) for j in (0, ey - 1) for i in range(ex)]
    inner = [(i, j) for j in range(1, ey - 1) for i in range(ex)]
    blocks = corners + inner

    fetches = [
        pltpu.make_async_copy(src, dst, in_sem.at[k])
        for k, (src, dst) in enumerate(
            [
                (sig_hbm, sig), (live_hbm, live_rows), (edge_hbm, bound_rows), (tdir_hbm, tdir),
                (tmask_hbm, tmask), (coef_hbm, coef),
            ]
        )
    ]
    for copy in fetches:
        copy.start()
    tile_groups = tile_sem.shape[0]
    span = ey // tile_groups

    def tile_copy(k):
        part = pl.ds(k * span, span)
        return pltpu.make_async_copy(tiles_hbm.at[:, part], tiles.at[:, part], tile_sem.at[k])

    for k in range(tile_groups):
        tile_copy(k).start()

    for r in range(DEG):
        for ref in (x_in[r], z_in[r], c_in[r]):
            ref[...] = jnp.zeros(ref.shape, ref.dtype)
    for k in range(len(cells)):
        cells[k][ZERO] = jnp.zeros(cells[k].shape[1:], bf)

    barrier = pltpu.get_barrier_semaphore()

    def around(dx, dy):
        px, py = gx + dx, gy + dy
        px = jnp.where(px >= nx, px - nx, jnp.where(px < 0, px + nx, px)) if dx else px
        py = jnp.where(py >= ny, py - ny, py) if dy else py
        return px, py

    def signal(semaphore, device):
        pl.semaphore_signal(semaphore, inc=1, device_id=device, device_id_type=MESH)

    def inside(dx, dy):
        ok = None
        for d, g, m in ((dx, gx, nx), (dy, gy, ny)):
            if d:
                here = g > 0 if d < 0 else g < m - 1
                ok = here if ok is None else jnp.logical_and(ok, here)
        return ok

    def flat(i, j):
        return j * ex + i

    for dx in (-1, 1):
        for dy in (-1, 0, 1):

            @pl.when(inside(dx, dy))
            def _():
                signal(barrier, (gx + dx, gy + dy))

    for dy in range(1, ny):
        signal(barrier, around(0, dy))
    for dx in (-FAR, FAR):
        signal(barrier, around(dx, 0))

    def near(g, m):
        return (g > 0).astype(jnp.int32) + (g < m - 1).astype(jnp.int32)

    greeted = near(gx, nx) * (1 + near(gy, ny)) + (ny - 1) + 2

    fetches[0].wait()
    for copy in fetches[1:3]:
        copy.wait()

    lane = lax.broadcasted_iota(jnp.int32, (1, size), 1)
    group = [
        jnp.logical_and(lane >= s * EDGE, lane < (s + 1) * EDGE).astype(bf) for s in range(groups)
    ]

    def repeats_of(i, j):
        return ((lane & (EDGE - 1)) < bound_rows[i, j]).astype(f32)

    def live_of(i, j):
        return (lane < live_rows[i, j]).astype(f32)

    def repeat(v):
        step = EDGE
        while step < size:
            v = v + pltpu.roll(v, step, 1)
            step *= 2
        return v

    def edge_of(i, j):
        return (lane < bound_rows[i, j]).astype(f32)

    first_row = lax.broadcasted_iota(jnp.int32, (chan, size), 0) == 0

    def prepare(i, j):
        b = flat(i, j)
        live = live_of(i, j)
        v = sig[i, j] * live
        cheb[0, b] = v
        own[0][b, :chan] = v.astype(bf)
        own[0][b, chan:] = jnp.where(first_row, live, 0.0).astype(bf)
        cells[0][b, :chan] = repeat((v * edge_of(i, j)).astype(bf))
        cells[0][b, chan:] = jnp.where(first_row, repeats_of(i, j), 0.0).astype(bf)

    def message(r, k):
        dx, dy = SIDES[k]
        now = cells[min(r, 1 + (r + 1) % 2)]
        x = 0 if dx < 0 else 1
        y = 0 if dy < 0 else 1
        if dy == 0:
            src, dst = x_out[r].at[x], x_in[r].at[1 - x]
        elif dx == 0:
            src, dst = now.at[pl.ds(flat(0, y * (ey - 1)), ex)], z_in[r].at[1 - y]
        else:
            src = now.at[flat(x * (ex - 1), y * (ey - 1))]
            dst = c_in[r].at[2 * (1 - x) + 1 - y]
        return pltpu.make_async_remote_copy(
            src_ref=src,
            dst_ref=dst,
            send_sem=send_sem.at[k],
            recv_sem=recv_sem.at[r % 2, k],
            device_id=(gx + dx, gy + dy),
            device_id_type=MESH,
        )

    def each(chosen, act, sign):
        for k in chosen:
            dx, dy = SIDES[k]

            @pl.when(inside(sign * dx, sign * dy))
            def _():
                act(k)

    x_sides, z_sides, c_sides = (0, 1), (2, 3), (4, 5, 6, 7)

    def send(r, chosen):
        each(chosen, lambda k: message(r, k).start(), 1)

    def sent(r):
        each(c_sides + z_sides + x_sides, lambda k: message(r, k).wait_send(), 1)

    def receive(r, chosen):
        each(chosen, lambda k: message(r, k).wait_recv(), -1)

    def cells_of(r):
        return cells[min(r, 1 + (r + 1) % 2)]

    def pack(r):
        for side in range(2):
            i = side * (ex - 1)
            for q in range(quads):
                packed = None
                for t in range(groups):
                    term = cells_of(r)[flat(i, q * groups + t)] * group[t]
                    packed = term if packed is None else packed + term
                x_out[r][side, q] = packed

    def unpack_x(r):
        for side in range(2):
            for q in range(quads):
                v = x_in[r][side, q]
                at = X_BASE + (side * quads + q) * groups
                cells_of(r)[at] = v
                for t in range(1, groups):
                    cells_of(r)[at + t] = pltpu.roll(v, t * EDGE, 1)

    def unpack_zc(r):
        for y in range(2):
            for i in range(ex):
                cells_of(r)[Z_BASE + y * ex + i] = z_in[r][y, i]
        for k in range(4):
            cells_of(r)[C_BASE + k] = c_in[r][k]

    def tables(i, j):
        b = flat(i, j)
        for s in range(slots):
            d = tdir[i, s, j]
            live = tmask[i, s, j] == 1
            row = (d * 11) >> 5
            ti = row + (i - 1)
            tj = d - 3 * row + (j - 1)
            at = tj * ex + ti
            up, down = ti < 0, ti > ex - 1
            at_x = X_BASE + (tj >> 2) * groups + ((s - tj) & 3)
            at = jnp.where(up, at_x, jnp.where(down, at_x + quads * groups, at))
            if j in (0, ey - 1):
                y = 0 if j == 0 else 1
                out = tj < 0 if j == 0 else tj > ey - 1
                at_z = Z_BASE + y * ex + ti
                at_z = jnp.where(up, C_BASE + y, jnp.where(down, C_BASE + 2 + y, at_z))
                at = jnp.where(out, at_z, at)
            mine = jnp.logical_and(live, d == 4)
            index[b * slots + s] = jnp.where(jnp.logical_and(live, d != 4), at, ZERO)
            used[b * slots + s] = jnp.where(mine, 1.0, 0.0)

    def weights(i, j):
        packed = None
        for s in range(slots):
            tile = tiles[i, j, s]
            term = (pltpu.roll(tile, s * EDGE, 1) if s else tile) * group[s]
            packed = term if packed is None else packed + term
        w_edge[flat(i, j), :size] = packed
        for t in range(groups):
            w_edge[flat(i, j), pl.ds(size + t * EDGE, EDGE)] = packed[:EDGE]

    def own_product(r, i, j):
        b = flat(i, j)
        mine = own[min(r, 1)][b]
        total = None
        for s in range(0, slots, 2):
            pair = jnp.concatenate(
                [mine * used[b * slots + s + k].astype(bf) for k in range(2)], axis=1
            )
            tile = jnp.concatenate([tiles[i, j, s + k] for k in range(2)], axis=1)
            term = lax.dot_general(pair, tile, NT, preferred_element_type=f32)
            total = term if total is None else total + term
        if r == 0:
            acc[b, : 2 * chan] = total
            acc[b, 2 * chan :] = repeat(total * edge_of(i, j))
            copies[b] = repeat(cheb[0, b] * edge_of(i, j))
        else:
            base = 2.0 * (slope[b] * cheb[r, b] - scale[b] * total) - cheb[r - 1, b]
            acc[b, :chan] = base
            if r < DEG - 1:
                acc[b, 2 * chan : 3 * chan] = repeat(base * edge_of(i, j))

    def edge_product(r, i, j):
        b = flat(i, j)
        picked = None
        for s in range(slots):
            term = cells_of(r)[index[b * slots + s]] * group[s]
            picked = term if picked is None else picked + term
        weight = w_edge[b] if r < DEG - 1 else w_edge[b, :size]
        return lax.dot_general(picked, weight, NT, preferred_element_type=f32)

    def add_totals(k):
        for s in range(scales):
            c = coef[s, k] * (0.5 if k == 0 else 1.0)
            for i, j in blocks:
                term = c * cheb[k, flat(i, j)]
                totals[s, i, j] = term if k == 0 else totals[s, i, j] + term

    sums = [None] * scales

    def advance(r, i, j):
        b = flat(i, j)
        edge = edge_product(r, i, j)
        if r == 0:
            adj = acc[b, : 2 * chan] + edge[:, :size]
            s = factor * live_of(i, j)
            m = s * adj[chan : chan + 1] - 1.0
            scale[b] = s
            slope[b] = m
            following = m * cheb[0, b] - s * adj[:chan]
            adj = acc[b, 2 * chan :] + edge[:, size:]
            s = factor * repeats_of(i, j)
            m = s * adj[chan : chan + 1] - 1.0
            cells_of(r + 1)[b] = (m * copies[b] - s * adj[:chan]).astype(bf)
        else:
            following = acc[b, :chan] - (2.0 * scale[b]) * edge[:, :size]
            if r < DEG - 1:
                far = acc[b, 2 * chan : 3 * chan] - (2.0 * factor * repeats_of(i, j)) * edge[:, size:]
                cells_of(r + 1)[b] = far.astype(bf)
        cheb[r + 1, b] = following
        if r < DEG - 1:
            own[1][b] = following.astype(bf)
        else:
            for s in range(scales):
                t = totals[s, i, j] + coef[s, DEG] * following
                sums[s] = t * t if sums[s] is None else sums[s] + t * t

    for i, j in corners:
        prepare(i, j)
    for i, j in inner:
        prepare(i, j)
    pack(0)
    pl.semaphore_wait(barrier, greeted)
    send(0, c_sides)
    send(0, z_sides)
    send(0, x_sides)
    for copy in fetches[3:]:
        copy.wait()
    factor = 2.0 / jnp.full((1, size), bound[0], f32)
    for i, j in blocks:
        tables(i, j)
    for r in range(DEG):
        if r == 0:
            for k in range(tile_groups):
                tile_copy(k).wait()
            for i, j in blocks:
                weights(i, j)
        for i, j in blocks:
            own_product(r, i, j)
        add_totals(r)
        receive(r, x_sides)
        sent(r)
        unpack_x(r)
        for i, j in inner:
            advance(r, i, j)
        receive(r, z_sides + c_sides)
        if r > 0:
            pl.semaphore_wait(know_sem.at[r - 1], len(JUMPS[r - 1]))
        if r < len(JUMPS):
            for dx in JUMPS[r]:
                signal(know_sem.at[r], around(dx, 0))
        unpack_zc(r)
        for i, j in corners:
            advance(r, i, j)
        if r < DEG - 1:
            send(r + 1, c_sides)
            send(r + 1, z_sides)
            pack(r + 1)
            send(r + 1, x_sides)

    width = en_in.shape[2]
    if width > scales * chan:
        sums.append(jnp.zeros((width - scales * chan, size), f32))
    stacked = jnp.concatenate(sums, axis=0)
    high = stacked.astype(bf)
    low = (stacked - high.astype(f32)).astype(bf)
    local = lax.dot_general(
        jnp.ones((chan, 2 * size), bf), jnp.concatenate([high, low], axis=1), NT,
        preferred_element_type=f32,
    )
    en_in[me] = local[:1]

    def share(px, py):
        return pltpu.make_async_remote_copy(
            src_ref=en_in.at[me],
            dst_ref=en_in.at[me],
            send_sem=en_sem.at[0],
            recv_sem=en_sem.at[1],
            device_id=(px, py),
            device_id_type=MESH,
        )

    for py in range(ny):

        @pl.when(gy != py)
        def _():
            share(gx, py).start()

        @pl.loop(1, nx, unroll=True)
        def _(kx):
            px = gx + kx
            share(jnp.where(px >= nx, px - nx, px), py).start()

    for s in range(scales):
        c = coef[s, DEG]
        for i, j in blocks:
            totals[s, i, j] = totals[s, i, j] + c * cheb[DEG, flat(i, j)]

    rest = en_in.at[pl.ds(0, n - 1)]
    pltpu.make_async_copy(rest, rest, en_sem.at[1]).wait()
    pltpu.make_async_copy(rest, rest, en_sem.at[0]).wait()


def hand_out(count, made, shared, out_hbm, energy_out, energy, sem):
    scales, chan = energy.shape
    stores = [pltpu.make_async_copy(made, out_hbm, sem.at[0])]
    stores[0].start()
    total = jnp.sum(shared[...], axis=0) * (1.0 / count)
    for s in range(scales):
        energy[s : s + 1, :] = total[:, s * chan : (s + 1) * chan]
    stores.append(pltpu.make_async_copy(energy, energy_out, sem.at[1]))
    stores[-1].start()
    for store in stores:
        store.wait()


def solution(mesh):
    nx, ny = mesh.shape["gx"], mesh.shape["gy"]
    n = nx * ny

    def shards(
        signals, tiles, tile_dir, tile_mask, live_rows, bound_rows, scale_coeffs, spectral_bound
    ):
        ex, ey, chan, size = signals.shape
        slots = tiles.shape[2]
        scales = scale_coeffs.shape[0]
        nb = ex * ey
        width = -(-scales * chan // 128) * 128
        quads = ey * EDGE // size
        bf, f32 = jnp.bfloat16, jnp.float32
        vmem = pl.BlockSpec(memory_space=pltpu.VMEM)
        hbm = pl.BlockSpec(memory_space=pltpu.HBM)
        rows = [chan * (2 if r == 0 else 1) for r in range(DEG)]
        made, shared = pl.pallas_call(
            functools.partial(kernel, nx, ny),
            out_shape=(
                jax.ShapeDtypeStruct((scales, ex, ey, chan, size), f32),
                jax.ShapeDtypeStruct((n, 1, width), f32),
            ),
            in_specs=[hbm] * 7 + [pl.BlockSpec(memory_space=pltpu.SMEM)],
            out_specs=(vmem, vmem),
            scratch_shapes=[
                pltpu.VMEM(signals.shape, f32),
                pltpu.SMEM((ex, slots, ey), jnp.int32),
                pltpu.SMEM((ex, slots, ey), jnp.int32),
                pltpu.SMEM((ex, ey), jnp.int32),
                pltpu.SMEM((ex, ey), jnp.int32),
                pltpu.SMEM(scale_coeffs.shape, f32),
                pltpu.SMEM((nb * slots,), jnp.int32),
                pltpu.SMEM((nb * slots,), f32),
                pltpu.VMEM((ex, ey, slots, size, size), bf),
                pltpu.VMEM((nb, 2 * size, size), bf),
                [pltpu.VMEM((nb, 2 * chan, size), bf), pltpu.VMEM((nb, chan, size), bf)],
                pltpu.VMEM((nb, 4 * chan, size), f32),
                pltpu.VMEM((nb, chan, size), f32),
                pltpu.VMEM((DEG + 1, nb, chan, size), f32),
                pltpu.VMEM((nb, 1, size), f32),
                pltpu.VMEM((nb, 1, size), f32),
                [pltpu.VMEM((ZERO + 1, rows[min(k, 1)], size), bf) for k in range(3)],
                [pltpu.VMEM((2, quads, rows[r], size), bf) for r in range(DEG)],
                [pltpu.VMEM((2, quads, rows[r], size), bf) for r in range(DEG)],
                [pltpu.VMEM((2, ex, rows[r], size), bf) for r in range(DEG)],
                [pltpu.VMEM((4, rows[r], size), bf) for r in range(DEG)],
                pltpu.SemaphoreType.DMA((6,)),
                pltpu.SemaphoreType.DMA((4,)),
                pltpu.SemaphoreType.DMA((8,)),
                pltpu.SemaphoreType.DMA((2, 8)),
                pltpu.SemaphoreType.DMA((2,)),
                pltpu.SemaphoreType.REGULAR((len(JUMPS),)),
            ],
            compiler_params=pltpu.CompilerParams(
                collective_id=0, has_side_effects=True, vmem_limit_bytes=VMEM_LIMIT
            ),
        )(
            *[
                pltpu.with_memory_space_constraint(a, pltpu.HBM)
                for a in (
                    signals, tiles, jnp.swapaxes(tile_dir, 1, 2), jnp.swapaxes(tile_mask, 1, 2),
                    live_rows, bound_rows, scale_coeffs,
                )
            ], spectral_bound
        )
        return pl.pallas_call(
            functools.partial(hand_out, n * nb * size),
            out_shape=(
                jax.ShapeDtypeStruct(made.shape, f32),
                jax.ShapeDtypeStruct((scales, chan), f32),
            ),
            in_specs=[vmem] * 2,
            out_specs=(hbm, hbm),
            scratch_shapes=[
                pltpu.VMEM((scales, chan), f32),
                pltpu.SemaphoreType.DMA((2,)),
            ],
            compiler_params=pltpu.CompilerParams(vmem_limit_bytes=VMEM_LIMIT),
        )(made, shared)

    placed = (
        P("gx", "gy", None, None),
        P("gx", "gy", None, None, None),
        P("gx", "gy", None),
        P("gx", "gy", None),
        P("gx", "gy"),
        P("gx", "gy"),
        P(),
        P(),
    )
    return jax.shard_map(
        shards,
        mesh=mesh,
        in_specs=placed,
        out_specs=(P(None, "gx", "gy", None, None), P()),
        check_vma=False,
    )
```

```python
import functools

import jax
import jax.numpy as jnp
from jax import lax
from jax.experimental import pallas as pl
from jax.experimental.pallas import tpu as pltpu
from jax.sharding import PartitionSpec as P

DEG = 4
EDGE = 32
VMEM_LIMIT = 24 * 1024 * 1024
MESH = pl.DeviceIdType.MESH
NT = (((1,), (1,)), ((), ()))
SIDES = ((-1, 0), (1, 0), (0, -1), (0, 1), (-1, -1), (-1, 1), (1, -1), (1, 1))
STEPS = (2, 4, 8, 16)
GROUPS = 2
X_BASE, Z_BASE, C_BASE, ZERO = 16, 32, 36, 40


def kernel(
    nx, ny, sig_hbm, tiles_hbm, tdir_hbm, tmask_hbm, live_hbm, edge_hbm, coef_hbm, bound,
    totals, en_in,
    sig, tdir, tmask, live_rows, bound_rows, coef, index, used, tiles, w_edge, own, acc,
    copies, cheb, slope, scale, cells, x_out, x_in, zc_in,
    in_sem, send_sem, recv_sem, en_sem, know_sem,
):
    ex, ey, chan, size = sig.shape
    slots = tiles.shape[2]
    scales = coef.shape[0]
    groups = size // EDGE
    wide = own[0].shape[1]
    quads = ey // groups
    n = nx * ny
    bf, f32 = jnp.bfloat16, jnp.float32
    gx, gy = lax.axis_index("gx"), lax.axis_index("gy")
    me = gx * ny + gy
    corners = [(i, j) for j in (0, ey - 1) for i in range(ex)]
    inner = [(i, j) for j in range(1, ey - 1) for i in range(ex)]
    blocks = corners + inner

    def landing(r, k):
        dx, dy = SIDES[k]
        x = 0 if dx < 0 else 1
        y = 0 if dy < 0 else 1
        if dy == 0:
            return x_in[r].at[x]
        if dx == 0:
            return zc_in[r].at[pl.ds(y * ex, ex)]
        return zc_in[r].at[pl.ds(2 * ex + 2 * x + y, 1)]

    def inside(dx, dy):
        ok = None
        for d, g, m in ((dx, gx, nx), (dy, gy, ny)):
            if d:
                here = g > 0 if d < 0 else g < m - 1
                ok = here if ok is None else jnp.logical_and(ok, here)
        return ok

    def signal(semaphore, device):
        pl.semaphore_signal(semaphore, inc=1, device_id=device, device_id_type=MESH)

    def flat(i, j):
        return j * ex + i

    fetches = [
        pltpu.make_async_copy(src, dst, in_sem.at[k])
        for src, dst, k in (
            (sig_hbm, sig, 0), (live_hbm, live_rows, 1), (edge_hbm, bound_rows, 1),
            (tdir_hbm, tdir, 2), (tmask_hbm, tmask, 2), (coef_hbm, coef, 2),
        )
    ]
    span = ey // GROUPS
    for k in range(GROUPS):
        part = pl.ds(k * span, span)
        fetches.append(
            pltpu.make_async_copy(tiles_hbm.at[:, part], tiles.at[:, part], in_sem.at[3 + k])
        )
    def near(g, m, step=1):
        return (g >= step).astype(jnp.int32) + (g < m - step).astype(jnp.int32)

    def tell(k):
        for dx in (-STEPS[k], STEPS[k]):

            @pl.when(gx >= -dx if dx < 0 else gx < nx - dx)
            def _():
                signal(know_sem.at[k], (gx + dx, gy))

    def hear(k):
        pl.semaphore_wait(know_sem.at[k], near(gx, nx, STEPS[k]))

    greeted = (1 + near(gx, nx)) * (1 + near(gy, ny)) - 1
    for copy in fetches[:3]:
        copy.start()
    barrier = pltpu.get_barrier_semaphore()
    for dx, dy in SIDES:

        @pl.when(inside(dx, dy))
        def _():
            signal(barrier, (gx + dx, gy + dy))

    for copy in fetches[3:]:
        copy.start()
    for k, (dx, dy) in enumerate(SIDES):

        @pl.when(jnp.logical_not(inside(dx, dy)))
        def _():
            for r in range(DEG):
                part = landing(r, k)
                part[...] = jnp.zeros(part.shape, bf)

    for k in range(len(cells)):
        cells[k][ZERO] = jnp.zeros(cells[k].shape[1:], bf)

    for copy in fetches[:3]:
        copy.wait()

    lane = lax.broadcasted_iota(jnp.int32, (1, size), 1)
    group = [
        jnp.logical_and(lane >= s * EDGE, lane < (s + 1) * EDGE).astype(bf) for s in range(groups)
    ]

    def repeats_of(i, j):
        return ((lane & (EDGE - 1)) < bound_rows[i, j]).astype(f32)

    def live_of(i, j):
        return (lane < live_rows[i, j]).astype(f32)

    def repeat(v):
        step = EDGE
        while step < size:
            v = v + pltpu.roll(v, step, 1)
            step *= 2
        return v

    def edge_of(i, j):
        return (lane < bound_rows[i, j]).astype(f32)

    first_row = lax.broadcasted_iota(jnp.int32, (wide - chan, size), 0) == 0

    def prepare(i, j):
        b = flat(i, j)
        live = live_of(i, j)
        v = sig[i, j] * live
        cheb[0, b] = v
        own[0][b, :chan] = v.astype(bf)
        own[0][b, chan:] = jnp.where(first_row, live, 0.0).astype(bf)
        cells[0][b, :chan] = repeat((v * edge_of(i, j)).astype(bf))
        cells[0][b, chan:] = jnp.where(first_row, repeats_of(i, j), 0.0).astype(bf)

    def message(r, k):
        dx, dy = SIDES[k]
        x = 0 if dx < 0 else 1
        y = 0 if dy < 0 else 1
        if dy == 0:
            src = x_out[r].at[x]
        elif dx == 0:
            src = cells_of(r).at[pl.ds(flat(0, y * (ey - 1)), ex)]
        else:
            src = cells_of(r).at[pl.ds(flat(x * (ex - 1), y * (ey - 1)), 1)]
        return pltpu.make_async_remote_copy(
            src_ref=src,
            dst_ref=landing(r, SIDES.index((-dx, -dy))),
            send_sem=send_sem.at[0],
            recv_sem=recv_sem.at[r % 2, 0 if dy == 0 else 1],
            device_id=(gx + dx, gy + dy),
            device_id_type=MESH,
        )

    x_sides, z_sides, c_sides = (0, 1), (2, 3), (4, 5, 6, 7)

    def send(r, chosen):
        for k in chosen:

            @pl.when(inside(*SIDES[k]))
            def _():
                message(r, k).start()

    x_both = jnp.logical_and(gx > 0, gx < nx - 1)
    y_both = jnp.logical_and(gy > 0, gy < ny - 1)

    def await_parts(ref, sem, counts):
        for xb in (True, False):
            for yb in (True, False):
                x_is = x_both if xb else jnp.logical_not(x_both)
                y_is = y_both if yb else jnp.logical_not(y_both)
                part = ref.at[pl.ds(0, counts(1 + xb, 1 + yb))]

                @pl.when(jnp.logical_and(x_is, y_is))
                def _():
                    pltpu.make_async_copy(part, part, sem).wait()

    def sent(r):
        await_parts(
            cells_of(r), send_sem.at[0], lambda xs, ys: quads * xs + ex * ys + xs * ys
        )

    def receive_x(r):
        for xb in (True, False):
            part = x_in[r].at[pl.ds(0, 1 + xb)]

            @pl.when(x_both if xb else jnp.logical_not(x_both))
            def _():
                pltpu.make_async_copy(part, part, recv_sem.at[r % 2, 0]).wait()

    def receive_zc(r):
        await_parts(zc_in[r], recv_sem.at[r % 2, 1], lambda xs, ys: ex * ys + xs * ys)

    def cells_of(r):
        return cells[min(r, 1 + (r + 1) % 2)]

    def pack(r):
        for side in range(2):
            i = side * (ex - 1)
            for q in range(quads):
                packed = None
                for t in range(groups):
                    term = cells_of(r)[flat(i, q * groups + t)] * group[t]
                    packed = term if packed is None else packed + term
                x_out[r][side, q] = packed

    def unpack_x(r):
        for side in range(2):
            for q in range(quads):
                v = x_in[r][side, q]
                at = X_BASE + (side * quads + q) * groups
                cells_of(r)[at] = v
                for t in range(1, groups):
                    cells_of(r)[at + t] = pltpu.roll(v, t * EDGE, 1)

    def unpack_zc(r):
        cells_of(r)[pl.ds(Z_BASE, 2 * ex + 4)] = zc_in[r][...]

    def tables(i, j):
        b = flat(i, j)
        for s in range(slots):
            d = tdir[i, s, j]
            live = tmask[i, s, j] == 1
            row = (d * 11) >> 5
            ti = row + (i - 1)
            tj = d - 3 * row + (j - 1)
            at = tj * ex + ti
            up, down = ti < 0, ti > ex - 1
            at_x = X_BASE + (tj >> 2) * groups + ((s - tj) & 3)
            at = jnp.where(up, at_x, jnp.where(down, at_x + quads * groups, at))
            if j in (0, ey - 1):
                y = 0 if j == 0 else 1
                out = tj < 0 if j == 0 else tj > ey - 1
                at_z = Z_BASE + y * ex + ti
                at_z = jnp.where(up, C_BASE + y, jnp.where(down, C_BASE + 2 + y, at_z))
                at = jnp.where(out, at_z, at)
            mine = jnp.logical_and(live, d == 4)
            index[b * slots + s] = jnp.where(jnp.logical_and(live, d != 4), at, ZERO)
            used[b * slots + s] = jnp.where(mine, 1.0, 0.0)

    def weights(i, j):
        packed = None
        for s in range(slots):
            tile = tiles[i, j, s]
            term = (pltpu.roll(tile, s * EDGE, 1) if s else tile) * group[s]
            packed = term if packed is None else packed + term
        w_edge[flat(i, j), :size] = packed
        for t in range(groups):
            w_edge[flat(i, j), pl.ds(size + t * EDGE, EDGE)] = packed[:EDGE]

    def own_product(r, i, j):
        b = flat(i, j)
        mine = own[min(r, 1)][b]
        total = None
        for s in range(0, slots, 2):
            pair = jnp.concatenate(
                [mine * used[b * slots + s + k].astype(bf) for k in range(2)], axis=1
            )
            tile = jnp.concatenate([tiles[i, j, s + k] for k in range(2)], axis=1)
            term = lax.dot_general(pair, tile, NT, preferred_element_type=f32)
            total = term if total is None else total + term
        if r == 0:
            acc[b, :wide] = total
            acc[b, wide:] = repeat(total * edge_of(i, j))
            copies[b] = repeat(cheb[0, b] * edge_of(i, j))
        else:
            base = 2.0 * (slope[b] * cheb[r, b] - scale[b] * total) - cheb[r - 1, b]
            acc[b, :chan] = base
            if r < DEG - 1:
                acc[b, wide : wide + chan] = repeat(base * edge_of(i, j))

    def edge_product(r, i, j):
        b = flat(i, j)
        picked = None
        for s in range(slots):
            term = cells_of(r)[index[b * slots + s]] * group[s]
            picked = term if picked is None else picked + term
        weight = w_edge[b] if r < DEG - 1 else w_edge[b, :size]
        return lax.dot_general(picked, weight, NT, preferred_element_type=f32)

    def add_totals(k):
        for s in range(scales):
            c = coef[s, k] * (0.5 if k == 0 else 1.0)
            for i, j in blocks:
                term = c * cheb[k, flat(i, j)]
                totals[s, i, j] = term if k == 0 else totals[s, i, j] + term

    sums = [None] * scales

    def advance(r, i, j):
        b = flat(i, j)
        edge = edge_product(r, i, j)
        if r == 0:
            adj = acc[b, :wide] + edge[:, :size]
            s = factor * live_of(i, j)
            m = s * adj[chan : chan + 1] - 1.0
            scale[b] = s
            slope[b] = m
            following = m * cheb[0, b] - s * adj[:chan]
            adj = acc[b, wide:] + edge[:, size:]
            s = factor * repeats_of(i, j)
            m = s * adj[chan : chan + 1] - 1.0
            cells_of(r + 1)[b] = (m * copies[b] - s * adj[:chan]).astype(bf)
        else:
            following = acc[b, :chan] - (2.0 * scale[b]) * edge[:, :size]
            if r < DEG - 1:
                far = acc[b, wide : wide + chan] - (2.0 * factor * repeats_of(i, j)) * edge[:, size:]
                cells_of(r + 1)[b] = far.astype(bf)
        cheb[r + 1, b] = following
        if r < DEG - 1:
            own[1][b] = following.astype(bf)
        else:
            for s in range(scales):
                t = totals[s, i, j] + coef[s, DEG] * following
                sums[s] = t * t if sums[s] is None else sums[s] + t * t

    for i, j in corners:
        prepare(i, j)
    for i, j in inner:
        prepare(i, j)
    pack(0)
    pl.semaphore_wait(barrier, greeted)
    send(0, x_sides)
    send(0, c_sides)
    send(0, z_sides)
    for copy in fetches[3:6]:
        copy.wait()
    factor = 2.0 / jnp.full((1, size), bound[0], f32)
    for r in range(DEG):
        if r == 0:
            for k in range(GROUPS):
                fetches[6 + k].wait()
                some = [(i, j) for j in range(k * span, (k + 1) * span) for i in range(ex)]
                for i, j in some:
                    tables(i, j)
                    weights(i, j)
                for i, j in some:
                    own_product(r, i, j)
        else:
            for i, j in blocks:
                own_product(r, i, j)
        add_totals(r)
        if r == DEG - 1:
            hear(r - 1)
            tell(r)
        receive_x(r)
        sent(r)
        unpack_x(r)
        for i, j in inner:
            advance(r, i, j)
        receive_zc(r)
        if r > 0:
            hear(r if r == DEG - 1 else r - 1)
        if r < DEG - 1:
            tell(r)
        unpack_zc(r)
        for i, j in corners:
            advance(r, i, j)
        if r < DEG - 1:
            send(r + 1, c_sides)
            pack(r + 1)
            send(r + 1, x_sides)
            send(r + 1, z_sides)

    width = en_in.shape[2]
    if width > scales * chan:
        sums.append(jnp.zeros((width - scales * chan, size), f32))
    stacked = jnp.concatenate(sums, axis=0)
    high = stacked.astype(bf)
    low = (stacked - high.astype(f32)).astype(bf)
    local = lax.dot_general(
        jnp.ones((chan, 2 * size), bf), jnp.concatenate([high, low], axis=1), NT,
        preferred_element_type=f32,
    )
    en_in[me] = local[:1]

    def share(px, py):
        return pltpu.make_async_remote_copy(
            src_ref=en_in.at[me],
            dst_ref=en_in.at[me],
            send_sem=en_sem.at[0],
            recv_sem=en_sem.at[1],
            device_id=(px, py),
            device_id_type=MESH,
        )

    for px in range(nx):

        @pl.when(me != px * ny)
        def _():
            share(px, 0).start()

    for py in range(1, ny):

        @pl.when(gy != py)
        def _():
            share(gx, py).start()

        @pl.loop(1, nx, unroll=True)
        def _(kx):
            px = gx + kx
            share(jnp.where(px >= nx, px - nx, px), py).start()

    for s in range(scales):
        c = coef[s, DEG]
        for i, j in blocks:
            totals[s, i, j] = totals[s, i, j] + c * cheb[DEG, flat(i, j)]

    rest = en_in.at[pl.ds(0, n - 1)]
    pltpu.make_async_copy(rest, rest, en_sem.at[1]).wait()
    pltpu.make_async_copy(rest, rest, en_sem.at[0]).wait()


def hand_out(count, made, shared, out_hbm, energy_out, energy, sem):
    scales, chan = energy.shape
    stores = [pltpu.make_async_copy(made, out_hbm, sem.at[0])]
    stores[0].start()
    total = jnp.sum(shared[...], axis=0) * (1.0 / count)
    for s in range(scales):
        energy[s : s + 1, :] = total[:, s * chan : (s + 1) * chan]
    stores.append(pltpu.make_async_copy(energy, energy_out, sem.at[1]))
    stores[-1].start(priority=1)
    for store in stores:
        store.wait()


def solution(mesh):
    nx, ny = mesh.shape["gx"], mesh.shape["gy"]
    n = nx * ny

    def shards(
        signals, tiles, tile_dir, tile_mask, live_rows, bound_rows, scale_coeffs, spectral_bound
    ):
        ex, ey, chan, size = signals.shape
        slots = tiles.shape[2]
        scales = scale_coeffs.shape[0]
        nb = ex * ey
        width = -(-scales * chan // 128) * 128
        quads = ey * EDGE // size
        bf, f32 = jnp.bfloat16, jnp.float32
        vmem = pl.BlockSpec(memory_space=pltpu.VMEM)
        hbm = pl.BlockSpec(memory_space=pltpu.HBM)
        rows = [chan + (8 if r == 0 else 0) for r in range(DEG)]
        made, shared = pl.pallas_call(
            functools.partial(kernel, nx, ny),
            out_shape=(
                jax.ShapeDtypeStruct((scales, ex, ey, chan, size), f32),
                jax.ShapeDtypeStruct((n, 1, width), f32),
            ),
            in_specs=[hbm] * 7 + [pl.BlockSpec(memory_space=pltpu.SMEM)],
            out_specs=(vmem, vmem),
            scratch_shapes=[
                pltpu.VMEM(signals.shape, f32),
                pltpu.SMEM((ex, slots, ey), jnp.int32),
                pltpu.SMEM((ex, slots, ey), jnp.int32),
                pltpu.SMEM((ex, ey), jnp.int32),
                pltpu.SMEM((ex, ey), jnp.int32),
                pltpu.SMEM(scale_coeffs.shape, f32),
                pltpu.SMEM((nb * slots,), jnp.int32),
                pltpu.SMEM((nb * slots,), f32),
                pltpu.VMEM((ex, ey, slots, size, size), bf),
                pltpu.VMEM((nb, 2 * size, size), bf),
                [pltpu.VMEM((nb, rows[k], size), bf) for k in range(2)],
                pltpu.VMEM((nb, 2 * rows[0], size), f32),
                pltpu.VMEM((nb, chan, size), f32),
                pltpu.VMEM((DEG + 1, nb, chan, size), f32),
                pltpu.VMEM((nb, 1, size), f32),
                pltpu.VMEM((nb, 1, size), f32),
                [pltpu.VMEM((ZERO + 1, rows[min(k, 1)], size), bf) for k in range(3)],
                [pltpu.VMEM((2, quads, rows[r], size), bf) for r in range(DEG)],
                [pltpu.VMEM((2, quads, rows[r], size), bf) for r in range(DEG)],
                [pltpu.VMEM((2 * ex + 4, rows[r], size), bf) for r in range(DEG)],
                pltpu.SemaphoreType.DMA((3 + GROUPS,)),
                pltpu.SemaphoreType.DMA((1,)),
                pltpu.SemaphoreType.DMA((2, 2)),
                pltpu.SemaphoreType.DMA((2,)),
                pltpu.SemaphoreType.REGULAR((len(STEPS),)),
            ],
            compiler_params=pltpu.CompilerParams(
                collective_id=0, has_side_effects=True, vmem_limit_bytes=VMEM_LIMIT
            ),
        )(
            *[
                pltpu.with_memory_space_constraint(a, pltpu.HBM)
                for a in (
                    signals, tiles, jnp.swapaxes(tile_dir, 1, 2), jnp.swapaxes(tile_mask, 1, 2),
                    live_rows, bound_rows, scale_coeffs,
                )
            ], spectral_bound
        )
        return pl.pallas_call(
            functools.partial(hand_out, n * nb * size),
            out_shape=(
                jax.ShapeDtypeStruct(made.shape, f32),
                jax.ShapeDtypeStruct((scales, chan), f32),
            ),
            in_specs=[vmem] * 2,
            out_specs=(hbm, hbm),
            scratch_shapes=[
                pltpu.VMEM((scales, chan), f32),
                pltpu.SemaphoreType.DMA((2,)),
            ],
            compiler_params=pltpu.CompilerParams(vmem_limit_bytes=VMEM_LIMIT),
        )(made, shared)

    placed = (
        P("gx", "gy", None, None),
        P("gx", "gy", None, None, None),
        P("gx", "gy", None),
        P("gx", "gy", None),
        P("gx", "gy"),
        P("gx", "gy"),
        P(),
        P(),
    )
    return jax.shard_map(
        shards,
        mesh=mesh,
        in_specs=placed,
        out_specs=(P(None, "gx", "gy", None, None), P()),
        check_vma=False,
    )
```

```python
import functools

import jax
import jax.numpy as jnp
from jax import lax
from jax.experimental import pallas as pl
from jax.experimental.pallas import tpu as pltpu
from jax.sharding import PartitionSpec as P

DEG = 4
EDGE = 32
VMEM_LIMIT = 24 * 1024 * 1024
MESH = pl.DeviceIdType.MESH
NT = (((1,), (1,)), ((), ()))
NN = (((1,), (0,)), ((), ()))
SIDES = ((-1, 0), (1, 0), (0, -1), (0, 1), (-1, -1), (-1, 1), (1, -1), (1, 1))
STEPS = (2, 4, 8, 16)
GROUPS = 2
X_BASE, Z_BASE, C_BASE, ZERO = 16, 32, 36, 40


def kernel(
    nx, ny, sig_hbm, tiles_hbm, tdir_hbm, tmask_hbm, live_hbm, edge_hbm, coef_hbm, bound,
    totals, en_in,
    sig, tdir, tmask, live_rows, bound_rows, coef, index, used, tiles, w_edge, own, acc,
    copies, cheb, slope, scale, cells, x_out, x_in, zc_in,
    in_sem, send_sem, recv_sem, en_sem, know_sem,
):
    ex, ey, chan, size = sig.shape
    slots = tiles.shape[2]
    scales = coef.shape[0]
    groups = size // EDGE
    wide = own[0].shape[1]
    quads = ey // groups
    n = nx * ny
    bf, f32 = jnp.bfloat16, jnp.float32
    gx, gy = lax.axis_index("gx"), lax.axis_index("gy")
    me = gx * ny + gy
    corners = [(i, j) for j in (0, ey - 1) for i in range(ex)]
    inner = [(i, j) for j in range(1, ey - 1) for i in range(ex)]
    blocks = corners + inner

    def landing(r, k):
        dx, dy = SIDES[k]
        x = 0 if dx < 0 else 1
        y = 0 if dy < 0 else 1
        if dy == 0:
            return x_in[r].at[x]
        if dx == 0:
            return zc_in[r].at[pl.ds(y * ex, ex)]
        return zc_in[r].at[pl.ds(2 * ex + 2 * x + y, 1)]

    def inside(dx, dy):
        ok = None
        for d, g, m in ((dx, gx, nx), (dy, gy, ny)):
            if d:
                here = g > 0 if d < 0 else g < m - 1
                ok = here if ok is None else jnp.logical_and(ok, here)
        return ok

    def signal(semaphore, device):
        pl.semaphore_signal(semaphore, inc=1, device_id=device, device_id_type=MESH)

    def flat(i, j):
        return j * ex + i

    fetches = [
        pltpu.make_async_copy(src, dst, in_sem.at[k])
        for src, dst, k in (
            (sig_hbm, sig, 0), (live_hbm, live_rows, 1), (edge_hbm, bound_rows, 1),
            (tdir_hbm, tdir, 2), (tmask_hbm, tmask, 2), (coef_hbm, coef, 2),
        )
    ]
    span = ey // GROUPS
    for k in range(GROUPS):
        part = pl.ds(k * span, span)
        fetches.append(
            pltpu.make_async_copy(tiles_hbm.at[:, part], tiles.at[:, part], in_sem.at[3 + k])
        )
    def near(g, m, step=1):
        return (g >= step).astype(jnp.int32) + (g < m - step).astype(jnp.int32)

    def tell(k):
        for dx in (-STEPS[k], STEPS[k]):

            @pl.when(gx >= -dx if dx < 0 else gx < nx - dx)
            def _():
                signal(know_sem.at[k], (gx + dx, gy))

    def hear(k):
        pl.semaphore_wait(know_sem.at[k], near(gx, nx, STEPS[k]))

    greeted = (1 + near(gx, nx)) * (1 + near(gy, ny)) - 1
    for copy in fetches[:3]:
        copy.start()
    barrier = pltpu.get_barrier_semaphore()
    for dx, dy in SIDES:

        @pl.when(inside(dx, dy))
        def _():
            signal(barrier, (gx + dx, gy + dy))

    for copy in fetches[3:]:
        copy.start()
    for k, (dx, dy) in enumerate(SIDES):

        @pl.when(jnp.logical_not(inside(dx, dy)))
        def _():
            for r in range(DEG):
                part = landing(r, k)
                part[...] = jnp.zeros(part.shape, bf)

    for k in range(len(cells)):
        cells[k][ZERO] = jnp.zeros(cells[k].shape[1:], bf)

    for copy in fetches[:3]:
        copy.wait()

    lane = lax.broadcasted_iota(jnp.int32, (1, size), 1)
    group = [
        jnp.logical_and(lane >= s * EDGE, lane < (s + 1) * EDGE).astype(bf) for s in range(groups)
    ]

    def repeats_of(i, j):
        return ((lane & (EDGE - 1)) < bound_rows[i, j]).astype(f32)

    def live_of(i, j):
        return (lane < live_rows[i, j]).astype(f32)

    def repeat(v):
        step = EDGE
        while step < size:
            v = v + pltpu.roll(v, step, 1)
            step *= 2
        return v

    def edge_of(i, j):
        return (lane < bound_rows[i, j]).astype(f32)

    first_row = lax.broadcasted_iota(jnp.int32, (wide - chan, size), 0) == 0

    def prepare(i, j):
        b = flat(i, j)
        live = live_of(i, j)
        v = sig[i, j] * live
        cheb[0, b] = v
        own[0][b, :chan] = v.astype(bf)
        own[0][b, chan:] = jnp.where(first_row, live, 0.0).astype(bf)
        cells[0][b, :chan] = repeat((v * edge_of(i, j)).astype(bf))
        cells[0][b, chan:] = jnp.where(first_row, repeats_of(i, j), 0.0).astype(bf)

    def message(r, k):
        dx, dy = SIDES[k]
        x = 0 if dx < 0 else 1
        y = 0 if dy < 0 else 1
        if dy == 0:
            src = x_out[r].at[x]
        elif dx == 0:
            src = cells_of(r).at[pl.ds(flat(0, y * (ey - 1)), ex)]
        else:
            src = cells_of(r).at[pl.ds(flat(x * (ex - 1), y * (ey - 1)), 1)]
        return pltpu.make_async_remote_copy(
            src_ref=src,
            dst_ref=landing(r, SIDES.index((-dx, -dy))),
            send_sem=send_sem.at[0],
            recv_sem=recv_sem.at[r % 2, 0 if dy == 0 else 1],
            device_id=(gx + dx, gy + dy),
            device_id_type=MESH,
        )

    x_sides, z_sides, c_sides = (0, 1), (2, 3), (4, 5, 6, 7)

    def send(r, chosen):
        for k in chosen:

            @pl.when(inside(*SIDES[k]))
            def _():
                message(r, k).start()

    x_both = jnp.logical_and(gx > 0, gx < nx - 1)
    y_both = jnp.logical_and(gy > 0, gy < ny - 1)

    def await_parts(ref, sem, counts):
        for xb in (True, False):
            for yb in (True, False):
                x_is = x_both if xb else jnp.logical_not(x_both)
                y_is = y_both if yb else jnp.logical_not(y_both)
                part = ref.at[pl.ds(0, counts(1 + xb, 1 + yb))]

                @pl.when(jnp.logical_and(x_is, y_is))
                def _():
                    pltpu.make_async_copy(part, part, sem).wait()

    def sent(r):
        await_parts(
            cells_of(r), send_sem.at[0], lambda xs, ys: quads * xs + ex * ys + xs * ys
        )

    def receive_x(r):
        for xb in (True, False):
            part = x_in[r].at[pl.ds(0, 1 + xb)]

            @pl.when(x_both if xb else jnp.logical_not(x_both))
            def _():
                pltpu.make_async_copy(part, part, recv_sem.at[r % 2, 0]).wait()

    def receive_zc(r):
        await_parts(zc_in[r], recv_sem.at[r % 2, 1], lambda xs, ys: ex * ys + xs * ys)

    def cells_of(r):
        return cells[min(r, 1 + (r + 1) % 2)]

    def pack(r):
        for side in range(2):
            i = side * (ex - 1)
            for q in range(quads):
                packed = None
                for t in range(groups):
                    term = cells_of(r)[flat(i, q * groups + t)] * group[t]
                    packed = term if packed is None else packed + term
                x_out[r][side, q] = packed

    def unpack_x(r):
        for side in range(2):
            for q in range(quads):
                v = x_in[r][side, q]
                at = X_BASE + (side * quads + q) * groups
                cells_of(r)[at] = v
                for t in range(1, groups):
                    cells_of(r)[at + t] = pltpu.roll(v, t * EDGE, 1)

    def unpack_zc(r):
        cells_of(r)[pl.ds(Z_BASE, 2 * ex + 4)] = zc_in[r][...]

    def tables(i, j):
        b = flat(i, j)
        for s in range(slots):
            d = tdir[i, s, j]
            live = tmask[i, s, j] == 1
            row = (d * 11) >> 5
            ti = row + (i - 1)
            tj = d - 3 * row + (j - 1)
            at = tj * ex + ti
            up, down = ti < 0, ti > ex - 1
            at_x = X_BASE + (tj >> 2) * groups + ((s - tj) & 3)
            at = jnp.where(up, at_x, jnp.where(down, at_x + quads * groups, at))
            if j in (0, ey - 1):
                y = 0 if j == 0 else 1
                out = tj < 0 if j == 0 else tj > ey - 1
                at_z = Z_BASE + y * ex + ti
                at_z = jnp.where(up, C_BASE + y, jnp.where(down, C_BASE + 2 + y, at_z))
                at = jnp.where(out, at_z, at)
            mine = jnp.logical_and(live, d == 4)
            index[b * slots + s] = jnp.where(jnp.logical_and(live, d != 4), at, ZERO)
            used[b * slots + s] = jnp.where(mine, 1.0, 0.0)

    def turn(packed):
        p = packed.astype(f32)
        q = jnp.concatenate([p[:EDGE]] * groups, axis=0)
        return jnp.concatenate([p.T.astype(bf), q.T.astype(bf)], axis=1)

    def weights(i, j):
        packed = None
        for s in range(slots):
            tile = tiles[i, j, s].astype(f32)
            rolled = pltpu.roll(tile, s * EDGE, 1) if s else tile
            packed = rolled if packed is None else jnp.where(lane >= s * EDGE, rolled, packed)
        w_edge[flat(i, j)] = turn(packed)

    def own_product(r, i, j):
        b = flat(i, j)
        mine = own[min(r, 1)][b]
        total = None
        for s in range(0, slots, 2):
            pair = jnp.concatenate(
                [mine * used[b * slots + s + k].astype(bf) for k in range(2)], axis=1
            )
            tile = jnp.concatenate([tiles[i, j, s + k] for k in range(2)], axis=1)
            term = lax.dot_general(pair, tile, NT, preferred_element_type=f32)
            total = term if total is None else total + term
        if r == 0:
            acc[b, :wide] = total
            acc[b, wide:] = repeat(total * edge_of(i, j))
            copies[b] = repeat(cheb[0, b] * edge_of(i, j))
        else:
            base = 2.0 * (slope[b] * cheb[r, b] - scale[b] * total) - cheb[r - 1, b]
            acc[b, :chan] = base
            if r < DEG - 1:
                acc[b, wide : wide + chan] = repeat(base * edge_of(i, j))

    def edge_product(r, i, j):
        b = flat(i, j)
        picked = None
        for s in range(slots):
            term = cells_of(r)[index[b * slots + s]] * group[s]
            picked = term if picked is None else picked + term
        weight = w_edge[b] if r < DEG - 1 else w_edge[b, :, :size]
        return lax.dot_general(picked, weight, NN, preferred_element_type=f32)

    def add_totals(k):
        for s in range(scales):
            c = coef[s, k] * (0.5 if k == 0 else 1.0)
            for i, j in blocks:
                term = c * cheb[k, flat(i, j)]
                totals[s, i, j] = term if k == 0 else totals[s, i, j] + term

    sums = [None] * scales

    def advance(r, i, j):
        b = flat(i, j)
        edge = edge_product(r, i, j)
        if r == 0:
            adj = acc[b, :wide] + edge[:, :size]
            s = factor * live_of(i, j)
            m = s * adj[chan : chan + 1] - 1.0
            scale[b] = s
            slope[b] = m
            following = m * cheb[0, b] - s * adj[:chan]
            adj = acc[b, wide:] + edge[:, size:]
            s = factor * repeats_of(i, j)
            m = s * adj[chan : chan + 1] - 1.0
            cells_of(r + 1)[b] = (m * copies[b] - s * adj[:chan]).astype(bf)
        else:
            following = acc[b, :chan] - (2.0 * scale[b]) * edge[:, :size]
            if r < DEG - 1:
                far = acc[b, wide : wide + chan] - (2.0 * factor * repeats_of(i, j)) * edge[:, size:]
                cells_of(r + 1)[b] = far.astype(bf)
        cheb[r + 1, b] = following
        if r < DEG - 1:
            own[1][b] = following.astype(bf)
        else:
            for s in range(scales):
                t = totals[s, i, j] + coef[s, DEG] * following
                sums[s] = t * t if sums[s] is None else sums[s] + t * t

    for i, j in corners:
        prepare(i, j)
    for i, j in inner:
        prepare(i, j)
    pack(0)
    pl.semaphore_wait(barrier, greeted)
    send(0, x_sides)
    send(0, c_sides)
    send(0, z_sides)
    for copy in fetches[3:6]:
        copy.wait()
    factor = 2.0 / jnp.full((1, size), bound[0], f32)
    for r in range(DEG):
        if r == 0:
            for k in range(GROUPS):
                fetches[6 + k].wait()
                some = [(i, j) for j in range(k * span, (k + 1) * span) for i in range(ex)]
                for i, j in some:
                    tables(i, j)
                    weights(i, j)
                for i, j in some:
                    own_product(r, i, j)
        else:
            for i, j in blocks:
                own_product(r, i, j)
        add_totals(r)
        if r == DEG - 1:
            hear(r - 1)
            tell(r)
        receive_x(r)
        sent(r)
        unpack_x(r)
        for i, j in inner:
            advance(r, i, j)
        receive_zc(r)
        if r > 0:
            hear(r if r == DEG - 1 else r - 1)
        if r < DEG - 1:
            tell(r)
        unpack_zc(r)
        for i, j in corners:
            advance(r, i, j)
        if r < DEG - 1:
            send(r + 1, c_sides)
            pack(r + 1)
            send(r + 1, x_sides)
            send(r + 1, z_sides)

    width = en_in.shape[2]
    if width > scales * chan:
        sums.append(jnp.zeros((width - scales * chan, size), f32))
    stacked = jnp.concatenate(sums, axis=0)
    high = stacked.astype(bf)
    low = (stacked - high.astype(f32)).astype(bf)
    local = lax.dot_general(
        jnp.ones((chan, 2 * size), bf), jnp.concatenate([high, low], axis=1), NT,
        preferred_element_type=f32,
    )
    en_in[me] = local[:1]

    def share(px, py):
        return pltpu.make_async_remote_copy(
            src_ref=en_in.at[me],
            dst_ref=en_in.at[me],
            send_sem=en_sem.at[0],
            recv_sem=en_sem.at[1],
            device_id=(px, py),
            device_id_type=MESH,
        )

    for px in range(nx):

        @pl.when(me != px * ny)
        def _():
            share(px, 0).start()

    for py in range(1, ny):

        @pl.when(gy != py)
        def _():
            share(gx, py).start()

        @pl.loop(1, nx, unroll=True)
        def _(kx):
            px = gx + kx
            share(jnp.where(px >= nx, px - nx, px), py).start()

    for s in range(scales):
        c = coef[s, DEG]
        for i, j in blocks:
            totals[s, i, j] = totals[s, i, j] + c * cheb[DEG, flat(i, j)]

    rest = en_in.at[pl.ds(0, n - 1)]
    pltpu.make_async_copy(rest, rest, en_sem.at[1]).wait()
    pltpu.make_async_copy(rest, rest, en_sem.at[0]).wait()


def hand_out(count, made, shared, out_hbm, energy_out, energy, sem):
    scales, chan = energy.shape
    stores = [pltpu.make_async_copy(made, out_hbm, sem.at[0])]
    stores[0].start()
    total = jnp.sum(shared[...], axis=0) * (1.0 / count)
    for s in range(scales):
        energy[s : s + 1, :] = total[:, s * chan : (s + 1) * chan]
    stores.append(pltpu.make_async_copy(energy, energy_out, sem.at[1]))
    stores[-1].start(priority=1)
    for store in stores:
        store.wait()


def solution(mesh):
    nx, ny = mesh.shape["gx"], mesh.shape["gy"]
    n = nx * ny

    def shards(
        signals, tiles, tile_dir, tile_mask, live_rows, bound_rows, scale_coeffs, spectral_bound
    ):
        ex, ey, chan, size = signals.shape
        slots = tiles.shape[2]
        scales = scale_coeffs.shape[0]
        nb = ex * ey
        width = -(-scales * chan // 128) * 128
        quads = ey * EDGE // size
        bf, f32 = jnp.bfloat16, jnp.float32
        vmem = pl.BlockSpec(memory_space=pltpu.VMEM)
        hbm = pl.BlockSpec(memory_space=pltpu.HBM)
        rows = [chan + (8 if r == 0 else 0) for r in range(DEG)]
        made, shared = pl.pallas_call(
            functools.partial(kernel, nx, ny),
            out_shape=(
                jax.ShapeDtypeStruct((scales, ex, ey, chan, size), f32),
                jax.ShapeDtypeStruct((n, 1, width), f32),
            ),
            in_specs=[hbm] * 7 + [pl.BlockSpec(memory_space=pltpu.SMEM)],
            out_specs=(vmem, vmem),
            scratch_shapes=[
                pltpu.VMEM(signals.shape, f32),
                pltpu.SMEM((ex, slots, ey), jnp.int32),
                pltpu.SMEM((ex, slots, ey), jnp.int32),
                pltpu.SMEM((ex, ey), jnp.int32),
                pltpu.SMEM((ex, ey), jnp.int32),
                pltpu.SMEM(scale_coeffs.shape, f32),
                pltpu.SMEM((nb * slots,), jnp.int32),
                pltpu.SMEM((nb * slots,), f32),
                pltpu.VMEM((ex, ey, slots, size, size), bf),
                pltpu.VMEM((nb, size, 2 * size), bf),
                [pltpu.VMEM((nb, rows[k], size), bf) for k in range(2)],
                pltpu.VMEM((nb, 2 * rows[0], size), f32),
                pltpu.VMEM((nb, chan, size), f32),
                pltpu.VMEM((DEG + 1, nb, chan, size), f32),
                pltpu.VMEM((nb, 1, size), f32),
                pltpu.VMEM((nb, 1, size), f32),
                [pltpu.VMEM((ZERO + 1, rows[min(k, 1)], size), bf) for k in range(3)],
                [pltpu.VMEM((2, quads, rows[r], size), bf) for r in range(DEG)],
                [pltpu.VMEM((2, quads, rows[r], size), bf) for r in range(DEG)],
                [pltpu.VMEM((2 * ex + 4, rows[r], size), bf) for r in range(DEG)],
                pltpu.SemaphoreType.DMA((3 + GROUPS,)),
                pltpu.SemaphoreType.DMA((1,)),
                pltpu.SemaphoreType.DMA((2, 2)),
                pltpu.SemaphoreType.DMA((2,)),
                pltpu.SemaphoreType.REGULAR((len(STEPS),)),
            ],
            compiler_params=pltpu.CompilerParams(
                collective_id=0, has_side_effects=True, vmem_limit_bytes=VMEM_LIMIT
            ),
        )(
            *[
                pltpu.with_memory_space_constraint(a, pltpu.HBM)
                for a in (
                    signals, tiles, jnp.swapaxes(tile_dir, 1, 2), jnp.swapaxes(tile_mask, 1, 2),
                    live_rows, bound_rows, scale_coeffs,
                )
            ], spectral_bound
        )
        return pl.pallas_call(
            functools.partial(hand_out, n * nb * size),
            out_shape=(
                jax.ShapeDtypeStruct(made.shape, f32),
                jax.ShapeDtypeStruct((scales, chan), f32),
            ),
            in_specs=[vmem] * 2,
            out_specs=(hbm, hbm),
            scratch_shapes=[
                pltpu.VMEM((scales, chan), f32),
                pltpu.SemaphoreType.DMA((2,)),
            ],
            compiler_params=pltpu.CompilerParams(vmem_limit_bytes=VMEM_LIMIT),
        )(made, shared)

    placed = (
        P("gx", "gy", None, None),
        P("gx", "gy", None, None, None),
        P("gx", "gy", None),
        P("gx", "gy", None),
        P("gx", "gy"),
        P("gx", "gy"),
        P(),
        P(),
    )
    return jax.shard_map(
        shards,
        mesh=mesh,
        in_specs=placed,
        out_specs=(P(None, "gx", "gy", None, None), P()),
        check_vma=False,
    )
```

```python
import functools

import jax
import jax.numpy as jnp
from jax import lax
from jax.experimental import pallas as pl
from jax.experimental.pallas import tpu as pltpu
from jax.sharding import PartitionSpec as P

DEG = 4
EDGE = 32
VMEM_LIMIT = 24 * 1024 * 1024
MESH = pl.DeviceIdType.MESH
NT = (((1,), (1,)), ((), ()))
NN = (((1,), (0,)), ((), ()))
SIDES = ((-1, 0), (1, 0), (0, -1), (0, 1), (-1, -1), (-1, 1), (1, -1), (1, 1))
STEPS = (2, 4, 8, 16)
GROUPS = 2
X_BASE, Z_BASE, C_BASE, ZERO = 16, 32, 36, 40


def kernel(
    nx, ny, sig_hbm, tiles_hbm, tdir_hbm, tmask_hbm, live_hbm, edge_hbm, coef_hbm, bound,
    totals, en_in,
    sig, tdir, tmask, live_rows, bound_rows, coef, index, used, tiles, w_edge, own, acc,
    copies, cheb, slope, scale, cells, x_out, x_in, zc_in,
    in_sem, send_sem, recv_sem, en_sem, know_sem,
):
    ex, ey, chan, size = sig.shape
    slots = tiles.shape[2]
    scales = coef.shape[0]
    groups = size // EDGE
    wide = own[0].shape[1]
    quads = ey // groups
    n = nx * ny
    bf, f32 = jnp.bfloat16, jnp.float32
    gx, gy = lax.axis_index("gx"), lax.axis_index("gy")
    me = gx * ny + gy
    corners = [(i, j) for j in (0, ey - 1) for i in range(ex)]
    inner = [(i, j) for j in range(1, ey - 1) for i in range(ex)]
    blocks = corners + inner

    def landing(r, k):
        dx, dy = SIDES[k]
        x = 0 if dx < 0 else 1
        y = 0 if dy < 0 else 1
        if dy == 0:
            return x_in[r].at[x]
        if dx == 0:
            return zc_in[r].at[pl.ds(y * ex, ex)]
        return zc_in[r].at[pl.ds(2 * ex + 2 * x + y, 1)]

    def inside(dx, dy):
        ok = None
        for d, g, m in ((dx, gx, nx), (dy, gy, ny)):
            if d:
                here = g > 0 if d < 0 else g < m - 1
                ok = here if ok is None else jnp.logical_and(ok, here)
        return ok

    def signal(semaphore, device):
        pl.semaphore_signal(semaphore, inc=1, device_id=device, device_id_type=MESH)

    def flat(i, j):
        return j * ex + i

    fetches = [
        pltpu.make_async_copy(src, dst, in_sem.at[k])
        for src, dst, k in (
            (sig_hbm, sig, 0), (live_hbm, live_rows, 0), (edge_hbm, bound_rows, 0),
            (tdir_hbm, tdir, 1), (tmask_hbm, tmask, 1), (coef_hbm, coef, 1),
        )
    ]
    span = ey // GROUPS
    for k in range(GROUPS):
        part = pl.ds(k * span, span)
        fetches.append(
            pltpu.make_async_copy(tiles_hbm.at[:, part], tiles.at[:, part], in_sem.at[1 + k])
        )
    def near(g, m, step=1):
        return (g >= step).astype(jnp.int32) + (g < m - step).astype(jnp.int32)

    def tell(k):
        for dx in (-STEPS[k], STEPS[k]):

            @pl.when(gx >= -dx if dx < 0 else gx < nx - dx)
            def _():
                signal(know_sem.at[k], (gx + dx, gy))

    def hear(k):
        pl.semaphore_wait(know_sem.at[k], near(gx, nx, STEPS[k]))

    greeted = (1 + near(gx, nx)) * (1 + near(gy, ny)) - 1
    for copy in fetches[:3]:
        copy.start()
    barrier = pltpu.get_barrier_semaphore()
    for dx, dy in SIDES:

        @pl.when(inside(dx, dy))
        def _():
            signal(barrier, (gx + dx, gy + dy))

    for copy in fetches[3:]:
        copy.start()
    for k, (dx, dy) in enumerate(SIDES):

        @pl.when(jnp.logical_not(inside(dx, dy)))
        def _():
            for r in range(DEG):
                part = landing(r, k)
                part[...] = jnp.zeros(part.shape, bf)

    for k in range(len(cells)):
        cells[k][ZERO] = jnp.zeros(cells[k].shape[1:], bf)

    for copy in fetches[:3]:
        copy.wait()

    lane = lax.broadcasted_iota(jnp.int32, (1, size), 1)
    group = [
        jnp.logical_and(lane >= s * EDGE, lane < (s + 1) * EDGE).astype(bf) for s in range(groups)
    ]

    def repeats_of(i, j):
        return ((lane & (EDGE - 1)) < bound_rows[i, j]).astype(f32)

    def live_of(i, j):
        return (lane < live_rows[i, j]).astype(f32)

    def repeat(v):
        step = EDGE
        while step < size:
            v = v + pltpu.roll(v, step, 1)
            step *= 2
        return v

    def edge_of(i, j):
        return (lane < bound_rows[i, j]).astype(f32)

    first_row = lax.broadcasted_iota(jnp.int32, (wide - chan, size), 0) == 0

    def prepare(i, j):
        b = flat(i, j)
        live = live_of(i, j)
        v = sig[i, j] * live
        cheb[0, b] = v
        own[0][b, :chan] = v.astype(bf)
        own[0][b, chan:] = jnp.where(first_row, live, 0.0).astype(bf)
        cells[0][b, :chan] = repeat((v * edge_of(i, j)).astype(bf))
        cells[0][b, chan:] = jnp.where(first_row, repeats_of(i, j), 0.0).astype(bf)

    def message(r, k):
        dx, dy = SIDES[k]
        x = 0 if dx < 0 else 1
        y = 0 if dy < 0 else 1
        if dy == 0:
            src = x_out[r].at[x]
        elif dx == 0:
            src = cells_of(r).at[pl.ds(flat(0, y * (ey - 1)), ex)]
        else:
            src = cells_of(r).at[pl.ds(flat(x * (ex - 1), y * (ey - 1)), 1)]
        return pltpu.make_async_remote_copy(
            src_ref=src,
            dst_ref=landing(r, SIDES.index((-dx, -dy))),
            send_sem=send_sem.at[0],
            recv_sem=recv_sem.at[r % 2, 0 if dy == 0 else 1],
            device_id=(gx + dx, gy + dy),
            device_id_type=MESH,
        )

    x_sides, z_sides, c_sides = (0, 1), (2, 3), (4, 5, 6, 7)

    def send(r, chosen):
        for k in chosen:

            @pl.when(inside(*SIDES[k]))
            def _():
                message(r, k).start()

    x_both = jnp.logical_and(gx > 0, gx < nx - 1)
    y_both = jnp.logical_and(gy > 0, gy < ny - 1)

    def await_parts(ref, sem, counts):
        for xb in (True, False):
            for yb in (True, False):
                x_is = x_both if xb else jnp.logical_not(x_both)
                y_is = y_both if yb else jnp.logical_not(y_both)
                part = ref.at[pl.ds(0, counts(1 + xb, 1 + yb))]

                @pl.when(jnp.logical_and(x_is, y_is))
                def _():
                    pltpu.make_async_copy(part, part, sem).wait()

    def sent(r):
        await_parts(
            cells_of(r), send_sem.at[0], lambda xs, ys: quads * xs + ex * ys + xs * ys
        )

    def receive_x(r):
        for xb in (True, False):
            part = x_in[r].at[pl.ds(0, 1 + xb)]

            @pl.when(x_both if xb else jnp.logical_not(x_both))
            def _():
                pltpu.make_async_copy(part, part, recv_sem.at[r % 2, 0]).wait()

    def receive_zc(r):
        await_parts(zc_in[r], recv_sem.at[r % 2, 1], lambda xs, ys: ex * ys + xs * ys)

    def cells_of(r):
        return cells[min(r, 1 + (r + 1) % 2)]

    def pack(r):
        for side in range(2):
            i = side * (ex - 1)
            for q in range(quads):
                packed = None
                for t in range(groups):
                    term = cells_of(r)[flat(i, q * groups + t)] * group[t]
                    packed = term if packed is None else packed + term
                x_out[r][side, q] = packed

    def unpack_x(r):
        for side in range(2):
            for q in range(quads):
                v = x_in[r][side, q]
                at = X_BASE + (side * quads + q) * groups
                cells_of(r)[at] = v
                for t in range(1, groups):
                    cells_of(r)[at + t] = pltpu.roll(v, t * EDGE, 1)

    def unpack_zc(r):
        cells_of(r)[pl.ds(Z_BASE, 2 * ex + 4)] = zc_in[r][...]

    def tables(i, j):
        b = flat(i, j)
        for s in range(slots):
            d = tdir[i, s, j]
            live = tmask[i, s, j] == 1
            row = (d * 11) >> 5
            ti = row + (i - 1)
            tj = d - 3 * row + (j - 1)
            at = tj * ex + ti
            up, down = ti < 0, ti > ex - 1
            at_x = X_BASE + (tj >> 2) * groups + ((s - tj) & 3)
            at = jnp.where(up, at_x, jnp.where(down, at_x + quads * groups, at))
            if j in (0, ey - 1):
                y = 0 if j == 0 else 1
                out = tj < 0 if j == 0 else tj > ey - 1
                at_z = Z_BASE + y * ex + ti
                at_z = jnp.where(up, C_BASE + y, jnp.where(down, C_BASE + 2 + y, at_z))
                at = jnp.where(out, at_z, at)
            mine = jnp.logical_and(live, d == 4)
            index[b * slots + s] = jnp.where(jnp.logical_and(live, d != 4), at, ZERO)
            used[b * slots + s] = jnp.where(mine, 1.0, 0.0)

    def turn(packed):
        p = packed.astype(f32)
        q = jnp.concatenate([p[:EDGE]] * groups, axis=0)
        return jnp.concatenate([p.T.astype(bf), q.T.astype(bf)], axis=1)

    def weights(i, j):
        packed = None
        for s in range(slots):
            tile = tiles[i, j, s].astype(f32)
            rolled = pltpu.roll(tile, s * EDGE, 1) if s else tile
            packed = rolled if packed is None else jnp.where(lane >= s * EDGE, rolled, packed)
        w_edge[flat(i, j)] = turn(packed)

    def own_product(r, i, j):
        b = flat(i, j)
        mine = own[min(r, 1)][b]
        total = None
        for s in range(0, slots, 2):
            pair = jnp.concatenate(
                [mine * used[b * slots + s + k].astype(bf) for k in range(2)], axis=1
            )
            tile = jnp.concatenate([tiles[i, j, s + k] for k in range(2)], axis=1)
            term = lax.dot_general(pair, tile, NT, preferred_element_type=f32)
            total = term if total is None else total + term
        if r == 0:
            acc[b, :wide] = total
            acc[b, wide:] = repeat(total * edge_of(i, j))
            copies[b] = repeat(cheb[0, b] * edge_of(i, j))
        else:
            base = 2.0 * (slope[b] * cheb[r, b] - scale[b] * total) - cheb[r - 1, b]
            acc[b, :chan] = base
            if r < DEG - 1:
                acc[b, wide : wide + chan] = repeat(base * edge_of(i, j))

    def edge_product(r, i, j):
        b = flat(i, j)
        picked = None
        for s in range(slots):
            term = cells_of(r)[index[b * slots + s]] * group[s]
            picked = term if picked is None else picked + term
        weight = w_edge[b] if r < DEG - 1 else w_edge[b, :, :size]
        return lax.dot_general(picked, weight, NN, preferred_element_type=f32)

    def add_totals(k):
        for s in range(scales):
            c = coef[s, k] * (0.5 if k == 0 else 1.0)
            for i, j in blocks:
                term = c * cheb[k, flat(i, j)]
                totals[s, i, j] = term if k == 0 else totals[s, i, j] + term

    sums = [None] * scales

    def advance(r, i, j):
        b = flat(i, j)
        edge = edge_product(r, i, j)
        if r == 0:
            adj = acc[b, :wide] + edge[:, :size]
            s = factor * live_of(i, j)
            m = s * adj[chan : chan + 1] - 1.0
            scale[b] = s
            slope[b] = m
            following = m * cheb[0, b] - s * adj[:chan]
            adj = acc[b, wide:] + edge[:, size:]
            s = factor * repeats_of(i, j)
            m = s * adj[chan : chan + 1] - 1.0
            cells_of(r + 1)[b] = (m * copies[b] - s * adj[:chan]).astype(bf)
        else:
            following = acc[b, :chan] - (2.0 * scale[b]) * edge[:, :size]
            if r < DEG - 1:
                far = acc[b, wide : wide + chan] - (2.0 * factor * repeats_of(i, j)) * edge[:, size:]
                cells_of(r + 1)[b] = far.astype(bf)
        cheb[r + 1, b] = following
        if r < DEG - 1:
            own[1][b] = following.astype(bf)
        else:
            for s in range(scales):
                t = totals[s, i, j] + coef[s, DEG] * following
                sums[s] = t * t if sums[s] is None else sums[s] + t * t

    for i, j in corners:
        prepare(i, j)
    for i, j in inner:
        prepare(i, j)
    pack(0)
    pl.semaphore_wait(barrier, greeted)
    send(0, c_sides)
    send(0, x_sides)
    send(0, z_sides)
    for copy in fetches[3:6]:
        copy.wait()
    factor = 2.0 / jnp.full((1, size), bound[0], f32)
    for r in range(DEG):
        if r == 0:
            for k in range(GROUPS):
                fetches[6 + k].wait()
                some = [(i, j) for j in range(k * span, (k + 1) * span) for i in range(ex)]
                for i, j in some:
                    tables(i, j)
                    weights(i, j)
                for i, j in some:
                    own_product(r, i, j)
        else:
            for i, j in blocks:
                own_product(r, i, j)
        add_totals(r)
        if r == DEG - 1:
            hear(r - 1)
            tell(r)
        receive_x(r)
        sent(r)
        unpack_x(r)
        for i, j in inner:
            advance(r, i, j)
        receive_zc(r)
        if r > 0:
            hear(r if r == DEG - 1 else r - 1)
        if r < DEG - 1:
            tell(r)
        unpack_zc(r)
        for i, j in corners:
            advance(r, i, j)
        if r < DEG - 1:
            send(r + 1, c_sides)
            pack(r + 1)
            send(r + 1, x_sides)
            send(r + 1, z_sides)

    width = en_in.shape[2]
    if width > scales * chan:
        sums.append(jnp.zeros((width - scales * chan, size), f32))
    stacked = jnp.concatenate(sums, axis=0)
    high = stacked.astype(bf)
    low = (stacked - high.astype(f32)).astype(bf)
    local = lax.dot_general(
        jnp.ones((chan, 2 * size), bf), jnp.concatenate([high, low], axis=1), NT,
        preferred_element_type=f32,
    )
    en_in[me] = local[:1]

    def share(px, py):
        return pltpu.make_async_remote_copy(
            src_ref=en_in.at[me],
            dst_ref=en_in.at[me],
            send_sem=send_sem.at[0],
            recv_sem=en_sem.at[0],
            device_id=(px, py),
            device_id_type=MESH,
        )

    for px in range(nx):

        @pl.when(me != px * ny)
        def _():
            share(px, 0).start()

    for py in range(1, ny):

        @pl.when(gy != py)
        def _():
            share(gx, py).start()

        @pl.loop(1, nx, unroll=True)
        def _(kx):
            px = gx + kx
            share(jnp.where(px >= nx, px - nx, px), py).start()

    for s in range(scales):
        c = coef[s, DEG]
        for i, j in blocks:
            totals[s, i, j] = totals[s, i, j] + c * cheb[DEG, flat(i, j)]

    rest = en_in.at[pl.ds(0, n - 1)]
    pltpu.make_async_copy(rest, rest, en_sem.at[0]).wait()
    pltpu.make_async_copy(rest, rest, send_sem.at[0]).wait()


def hand_out(count, made, shared, out_hbm, energy_out, energy, sem):
    scales, chan = energy.shape
    stores = [pltpu.make_async_copy(made, out_hbm, sem.at[0])]
    stores[0].start()
    total = jnp.sum(shared[...], axis=0) * (1.0 / count)
    for s in range(scales):
        energy[s : s + 1, :] = total[:, s * chan : (s + 1) * chan]
    stores.append(pltpu.make_async_copy(energy, energy_out, sem.at[1]))
    stores[-1].start(priority=1)
    for store in stores:
        store.wait()


def solution(mesh):
    nx, ny = mesh.shape["gx"], mesh.shape["gy"]
    n = nx * ny

    def shards(
        signals, tiles, tile_dir, tile_mask, live_rows, bound_rows, scale_coeffs, spectral_bound
    ):
        ex, ey, chan, size = signals.shape
        slots = tiles.shape[2]
        scales = scale_coeffs.shape[0]
        nb = ex * ey
        width = -(-scales * chan // 128) * 128
        quads = ey * EDGE // size
        bf, f32 = jnp.bfloat16, jnp.float32
        vmem = pl.BlockSpec(memory_space=pltpu.VMEM)
        hbm = pl.BlockSpec(memory_space=pltpu.HBM)
        rows = [chan + (8 if r == 0 else 0) for r in range(DEG)]
        made, shared = pl.pallas_call(
            functools.partial(kernel, nx, ny),
            out_shape=(
                jax.ShapeDtypeStruct((scales, ex, ey, chan, size), f32),
                jax.ShapeDtypeStruct((n, 1, width), f32),
            ),
            in_specs=[hbm] * 7 + [pl.BlockSpec(memory_space=pltpu.SMEM)],
            out_specs=(vmem, vmem),
            scratch_shapes=[
                pltpu.VMEM(signals.shape, f32),
                pltpu.SMEM((ex, slots, ey), jnp.int32),
                pltpu.SMEM((ex, slots, ey), jnp.int32),
                pltpu.SMEM((ex, ey), jnp.int32),
                pltpu.SMEM((ex, ey), jnp.int32),
                pltpu.SMEM(scale_coeffs.shape, f32),
                pltpu.SMEM((nb * slots,), jnp.int32),
                pltpu.SMEM((nb * slots,), f32),
                pltpu.VMEM((ex, ey, slots, size, size), bf),
                pltpu.VMEM((nb, size, 2 * size), bf),
                [pltpu.VMEM((nb, rows[k], size), bf) for k in range(2)],
                pltpu.VMEM((nb, 2 * rows[0], size), f32),
                pltpu.VMEM((nb, chan, size), f32),
                pltpu.VMEM((DEG + 1, nb, chan, size), f32),
                pltpu.VMEM((nb, 1, size), f32),
                pltpu.VMEM((nb, 1, size), f32),
                [pltpu.VMEM((ZERO + 1, rows[min(k, 1)], size), bf) for k in range(3)],
                [pltpu.VMEM((2, quads, rows[r], size), bf) for r in range(DEG)],
                [pltpu.VMEM((2, quads, rows[r], size), bf) for r in range(DEG)],
                [pltpu.VMEM((2 * ex + 4, rows[r], size), bf) for r in range(DEG)],
                pltpu.SemaphoreType.DMA((1 + GROUPS,)),
                pltpu.SemaphoreType.DMA((1,)),
                pltpu.SemaphoreType.DMA((2, 2)),
                pltpu.SemaphoreType.DMA((1,)),
                pltpu.SemaphoreType.REGULAR((len(STEPS),)),
            ],
            compiler_params=pltpu.CompilerParams(
                collective_id=0, has_side_effects=True, vmem_limit_bytes=VMEM_LIMIT
            ),
        )(
            *[
                pltpu.with_memory_space_constraint(a, pltpu.HBM)
                for a in (
                    signals, tiles, jnp.swapaxes(tile_dir, 1, 2), jnp.swapaxes(tile_mask, 1, 2),
                    live_rows, bound_rows, scale_coeffs,
                )
            ], spectral_bound
        )
        return pl.pallas_call(
            functools.partial(hand_out, n * nb * size),
            out_shape=(
                jax.ShapeDtypeStruct(made.shape, f32),
                jax.ShapeDtypeStruct((scales, chan), f32),
            ),
            in_specs=[vmem] * 2,
            out_specs=(hbm, hbm),
            scratch_shapes=[
                pltpu.VMEM((scales, chan), f32),
                pltpu.SemaphoreType.DMA((2,)),
            ],
            compiler_params=pltpu.CompilerParams(vmem_limit_bytes=VMEM_LIMIT),
        )(made, shared)

    placed = (
        P("gx", "gy", None, None),
        P("gx", "gy", None, None, None),
        P("gx", "gy", None),
        P("gx", "gy", None),
        P("gx", "gy"),
        P("gx", "gy"),
        P(),
        P(),
    )
    return jax.shard_map(
        shards,
        mesh=mesh,
        in_specs=placed,
        out_specs=(P(None, "gx", "gy", None, None), P()),
        check_vma=False,
    )
```

```python
import functools

import jax
import jax.numpy as jnp
from jax import lax
from jax.experimental import pallas as pl
from jax.experimental.pallas import tpu as pltpu
from jax.sharding import PartitionSpec as P

DEG = 4
EDGE = 32
VMEM_LIMIT = 24 * 1024 * 1024
MESH = pl.DeviceIdType.MESH
NT = (((1,), (1,)), ((), ()))
NN = (((1,), (0,)), ((), ()))
SIDES = ((-1, 0), (1, 0), (0, -1), (0, 1), (-1, -1), (-1, 1), (1, -1), (1, 1))
STEPS = (2, 4, 8, 16)
GROUPS = 2
X_BASE, Z_BASE, C_BASE, ZERO = 16, 32, 36, 40


def kernel(
    nx, ny, sig_hbm, tiles_hbm, tdir_hbm, tmask_hbm, live_hbm, edge_hbm, coef_hbm, bound,
    totals, en_in,
    sig, tdir, tmask, live_rows, bound_rows, coef, index, used, tiles, w_edge, own, acc,
    copies, cheb, slope, scale, cells, x_out, x_in, zc_in,
    in_sem, send_sem, recv_sem, en_sem, know_sem,
):
    ex, ey, chan, size = sig.shape
    slots = tiles.shape[2]
    scales = coef.shape[0]
    groups = size // EDGE
    wide = own[0].shape[1]
    quads = ey // groups
    n = nx * ny
    bf, f32 = jnp.bfloat16, jnp.float32
    gx, gy = lax.axis_index("gx"), lax.axis_index("gy")
    me = gx * ny + gy
    corners = [(i, j) for j in (0, ey - 1) for i in range(ex)]
    inner = [(i, j) for j in range(1, ey - 1) for i in range(ex)]
    blocks = corners + inner

    def landing(r, k):
        dx, dy = SIDES[k]
        x = 0 if dx < 0 else 1
        y = 0 if dy < 0 else 1
        if dy == 0:
            return x_in[r].at[x]
        if dx == 0:
            return zc_in[r].at[pl.ds(y * ex, ex)]
        return zc_in[r].at[pl.ds(2 * ex + 2 * x + y, 1)]

    def inside(dx, dy):
        ok = None
        for d, g, m in ((dx, gx, nx), (dy, gy, ny)):
            if d:
                here = g > 0 if d < 0 else g < m - 1
                ok = here if ok is None else jnp.logical_and(ok, here)
        return ok

    def signal(semaphore, device):
        pl.semaphore_signal(semaphore, inc=1, device_id=device, device_id_type=MESH)

    def flat(i, j):
        return j * ex + i

    fetches = [
        pltpu.make_async_copy(src, dst, in_sem.at[k])
        for src, dst, k in (
            (sig_hbm, sig, 0), (live_hbm, live_rows, 0), (edge_hbm, bound_rows, 0),
            (tdir_hbm, tdir, 1), (tmask_hbm, tmask, 1), (coef_hbm, coef, 1),
        )
    ]
    span = ey // GROUPS
    for k in range(GROUPS):
        part = pl.ds(k * span, span)
        fetches.append(
            pltpu.make_async_copy(tiles_hbm.at[:, part], tiles.at[:, part], in_sem.at[1 + k])
        )
    def near(g, m, step=1):
        return (g >= step).astype(jnp.int32) + (g < m - step).astype(jnp.int32)

    def tell(k):
        for dx in (-STEPS[k], STEPS[k]):

            @pl.when(gx >= -dx if dx < 0 else gx < nx - dx)
            def _():
                signal(know_sem.at[k], (gx + dx, gy))

    def hear(k):
        pl.semaphore_wait(know_sem.at[k], near(gx, nx, STEPS[k]))

    greeted = (1 + near(gx, nx)) * (1 + near(gy, ny)) - 1
    fetches[0].start()
    barrier = pltpu.get_barrier_semaphore()
    for dx, dy in SIDES:

        @pl.when(inside(dx, dy))
        def _():
            signal(barrier, (gx + dx, gy + dy))

    for copy in fetches[1:]:
        copy.start()
    for k, (dx, dy) in enumerate(SIDES):

        @pl.when(jnp.logical_not(inside(dx, dy)))
        def _():
            for r in range(DEG):
                part = landing(r, k)
                part[...] = jnp.zeros(part.shape, bf)

    for k in range(len(cells)):
        cells[k][ZERO] = jnp.zeros(cells[k].shape[1:], bf)

    for copy in fetches[:3]:
        copy.wait()

    lane = lax.broadcasted_iota(jnp.int32, (1, size), 1)
    group = [
        jnp.logical_and(lane >= s * EDGE, lane < (s + 1) * EDGE).astype(bf) for s in range(groups)
    ]

    def repeats_of(i, j):
        return ((lane & (EDGE - 1)) < bound_rows[i, j]).astype(f32)

    def live_of(i, j):
        return (lane < live_rows[i, j]).astype(f32)

    def repeat(v):
        step = EDGE
        while step < size:
            v = v + pltpu.roll(v, step, 1)
            step *= 2
        return v

    def edge_of(i, j):
        return (lane < bound_rows[i, j]).astype(f32)

    first_row = lax.broadcasted_iota(jnp.int32, (wide - chan, size), 0) == 0

    def prepare(i, j):
        b = flat(i, j)
        live = live_of(i, j)
        v = sig[i, j] * live
        cheb[0, b] = v
        own[0][b, :chan] = v.astype(bf)
        own[0][b, chan:] = jnp.where(first_row, live, 0.0).astype(bf)
        cells[0][b, :chan] = repeat((v * edge_of(i, j)).astype(bf))
        cells[0][b, chan:] = jnp.where(first_row, repeats_of(i, j), 0.0).astype(bf)

    def message(r, k):
        dx, dy = SIDES[k]
        x = 0 if dx < 0 else 1
        y = 0 if dy < 0 else 1
        if dy == 0:
            src = x_out[r].at[x]
        elif dx == 0:
            src = cells_of(r).at[pl.ds(flat(0, y * (ey - 1)), ex)]
        else:
            src = cells_of(r).at[pl.ds(flat(x * (ex - 1), y * (ey - 1)), 1)]
        return pltpu.make_async_remote_copy(
            src_ref=src,
            dst_ref=landing(r, SIDES.index((-dx, -dy))),
            send_sem=send_sem.at[0],
            recv_sem=recv_sem.at[r % 2, 0 if dy == 0 else 1],
            device_id=(gx + dx, gy + dy),
            device_id_type=MESH,
        )

    x_sides, z_sides, c_sides = (0, 1), (2, 3), (4, 5, 6, 7)

    def send(r, chosen):
        for k in chosen:

            @pl.when(inside(*SIDES[k]))
            def _():
                message(r, k).start()

    x_both = jnp.logical_and(gx > 0, gx < nx - 1)
    y_both = jnp.logical_and(gy > 0, gy < ny - 1)

    def await_parts(ref, sem, counts):
        for xb in (True, False):
            for yb in (True, False):
                x_is = x_both if xb else jnp.logical_not(x_both)
                y_is = y_both if yb else jnp.logical_not(y_both)
                part = ref.at[pl.ds(0, counts(1 + xb, 1 + yb))]

                @pl.when(jnp.logical_and(x_is, y_is))
                def _():
                    pltpu.make_async_copy(part, part, sem).wait()

    def sent(r):
        await_parts(
            cells_of(r), send_sem.at[0], lambda xs, ys: quads * xs + ex * ys + xs * ys
        )

    def receive_x(r):
        for xb in (True, False):
            part = x_in[r].at[pl.ds(0, 1 + xb)]

            @pl.when(x_both if xb else jnp.logical_not(x_both))
            def _():
                pltpu.make_async_copy(part, part, recv_sem.at[r % 2, 0]).wait()

    def receive_zc(r):
        await_parts(zc_in[r], recv_sem.at[r % 2, 1], lambda xs, ys: ex * ys + xs * ys)

    def cells_of(r):
        return cells[min(r, 1 + (r + 1) % 2)]

    def pack(r):
        for side in range(2):
            i = side * (ex - 1)
            for q in range(quads):
                packed = None
                for t in range(groups):
                    term = cells_of(r)[flat(i, q * groups + t)] * group[t]
                    packed = term if packed is None else packed + term
                x_out[r][side, q] = packed

    def unpack_x(r):
        for side in range(2):
            for q in range(quads):
                v = x_in[r][side, q]
                at = X_BASE + (side * quads + q) * groups
                cells_of(r)[at] = v
                for t in range(1, groups):
                    cells_of(r)[at + t] = pltpu.roll(v, t * EDGE, 1)

    def unpack_zc(r):
        cells_of(r)[pl.ds(Z_BASE, 2 * ex + 4)] = zc_in[r][...]

    def tables(i, j):
        b = flat(i, j)
        for s in range(slots):
            d = tdir[i, s, j]
            live = tmask[i, s, j] == 1
            row = (d * 11) >> 5
            ti = row + (i - 1)
            tj = d - 3 * row + (j - 1)
            at = tj * ex + ti
            up, down = ti < 0, ti > ex - 1
            at_x = X_BASE + (tj >> 2) * groups + ((s - tj) & 3)
            at = jnp.where(up, at_x, jnp.where(down, at_x + quads * groups, at))
            if j in (0, ey - 1):
                y = 0 if j == 0 else 1
                out = tj < 0 if j == 0 else tj > ey - 1
                at_z = Z_BASE + y * ex + ti
                at_z = jnp.where(up, C_BASE + y, jnp.where(down, C_BASE + 2 + y, at_z))
                at = jnp.where(out, at_z, at)
            mine = jnp.logical_and(live, d == 4)
            index[b * slots + s] = jnp.where(jnp.logical_and(live, d != 4), at, ZERO)
            used[b * slots + s] = jnp.where(mine, 1.0, 0.0)

    def turn(packed):
        p = packed.astype(f32)
        q = jnp.concatenate([p[:EDGE]] * groups, axis=0)
        return jnp.concatenate([p.T.astype(bf), q.T.astype(bf)], axis=1)

    def weights(i, j):
        packed = None
        for s in range(slots):
            tile = tiles[i, j, s].astype(f32)
            rolled = pltpu.roll(tile, s * EDGE, 1) if s else tile
            packed = rolled if packed is None else jnp.where(lane >= s * EDGE, rolled, packed)
        w_edge[flat(i, j)] = turn(packed)

    def own_product(r, i, j):
        b = flat(i, j)
        mine = own[min(r, 1)][b]
        total = None
        for s in range(0, slots, 2):
            pair = jnp.concatenate(
                [mine * used[b * slots + s + k].astype(bf) for k in range(2)], axis=1
            )
            tile = jnp.concatenate([tiles[i, j, s + k] for k in range(2)], axis=1)
            term = lax.dot_general(pair, tile, NT, preferred_element_type=f32)
            total = term if total is None else total + term
        if r == 0:
            acc[b, :wide] = total
            acc[b, wide:] = repeat(total * edge_of(i, j))
            copies[b] = repeat(cheb[0, b] * edge_of(i, j))
        else:
            base = 2.0 * (slope[b] * cheb[r, b] - scale[b] * total) - cheb[r - 1, b]
            acc[b, :chan] = base
            if r < DEG - 1:
                acc[b, wide : wide + chan] = repeat(base * edge_of(i, j))

    def edge_product(r, i, j):
        b = flat(i, j)
        picked = None
        for s in range(slots):
            term = cells_of(r)[index[b * slots + s]] * group[s]
            picked = term if picked is None else picked + term
        weight = w_edge[b] if r < DEG - 1 else w_edge[b, :, :size]
        return lax.dot_general(picked, weight, NN, preferred_element_type=f32)

    def add_totals(k):
        for s in range(scales):
            c = coef[s, k] * (0.5 if k == 0 else 1.0)
            for i, j in blocks:
                term = c * cheb[k, flat(i, j)]
                totals[s, i, j] = term if k == 0 else totals[s, i, j] + term

    sums = [None] * scales

    def advance(r, i, j):
        b = flat(i, j)
        edge = edge_product(r, i, j)
        if r == 0:
            adj = acc[b, :wide] + edge[:, :size]
            s = factor * live_of(i, j)
            m = s * adj[chan : chan + 1] - 1.0
            scale[b] = s
            slope[b] = m
            following = m * cheb[0, b] - s * adj[:chan]
            adj = acc[b, wide:] + edge[:, size:]
            s = factor * repeats_of(i, j)
            m = s * adj[chan : chan + 1] - 1.0
            cells_of(r + 1)[b] = (m * copies[b] - s * adj[:chan]).astype(bf)
        else:
            following = acc[b, :chan] - (2.0 * scale[b]) * edge[:, :size]
            if r < DEG - 1:
                far = acc[b, wide : wide + chan] - (2.0 * factor * repeats_of(i, j)) * edge[:, size:]
                cells_of(r + 1)[b] = far.astype(bf)
        cheb[r + 1, b] = following
        if r < DEG - 1:
            own[1][b] = following.astype(bf)
        else:
            for s in range(scales):
                t = totals[s, i, j] + coef[s, DEG] * following
                sums[s] = t * t if sums[s] is None else sums[s] + t * t

    for i, j in corners:
        prepare(i, j)
    for i, j in inner:
        prepare(i, j)
    pack(0)
    pl.semaphore_wait(barrier, greeted)
    send(0, c_sides)
    send(0, x_sides)
    send(0, z_sides)
    for copy in fetches[3:6]:
        copy.wait()
    factor = 2.0 / jnp.full((1, size), bound[0], f32)
    for r in range(DEG):
        if r == 0:
            for k in range(GROUPS):
                fetches[6 + k].wait()
                some = [(i, j) for j in range(k * span, (k + 1) * span) for i in range(ex)]
                for i, j in some:
                    tables(i, j)
                    weights(i, j)
                for i, j in some:
                    own_product(r, i, j)
        else:
            for i, j in blocks:
                own_product(r, i, j)
        add_totals(r)
        if r == DEG - 2:
            hear(r - 1)
            tell(r)
        receive_x(r)
        sent(r)
        unpack_x(r)
        for i, j in inner:
            advance(r, i, j)
        receive_zc(r)
        if r > 0:
            hear(r - 1 if r == 1 else r)
        if r < DEG - 1:
            tell(r + 1 if r == DEG - 2 else r)
        unpack_zc(r)
        for i, j in corners:
            advance(r, i, j)
        if r < DEG - 1:
            send(r + 1, c_sides)
            pack(r + 1)
            send(r + 1, x_sides)
            send(r + 1, z_sides)

    width = en_in.shape[2]
    if width > scales * chan:
        sums.append(jnp.zeros((width - scales * chan, size), f32))
    stacked = jnp.concatenate(sums, axis=0)
    high = stacked.astype(bf)
    low = (stacked - high.astype(f32)).astype(bf)
    local = lax.dot_general(
        jnp.ones((chan, 2 * size), bf), jnp.concatenate([high, low], axis=1), NT,
        preferred_element_type=f32,
    )
    en_in[me] = local[:1]

    def share(px, py):
        return pltpu.make_async_remote_copy(
            src_ref=en_in.at[me],
            dst_ref=en_in.at[me],
            send_sem=send_sem.at[0],
            recv_sem=en_sem.at[0],
            device_id=(px, py),
            device_id_type=MESH,
        )

    for px in range(nx):

        @pl.when(me != px * ny)
        def _():
            share(px, 0).start()

    for py in range(1, ny):

        @pl.when(gy != py)
        def _():
            share(gx, py).start()

        @pl.loop(1, nx, unroll=True)
        def _(kx):
            px = gx + kx
            share(jnp.where(px >= nx, px - nx, px), py).start()

    for s in range(scales):
        c = coef[s, DEG]
        for i, j in blocks:
            totals[s, i, j] = totals[s, i, j] + c * cheb[DEG, flat(i, j)]

    rest = en_in.at[pl.ds(0, n - 1)]
    pltpu.make_async_copy(rest, rest, en_sem.at[0]).wait()
    pltpu.make_async_copy(rest, rest, send_sem.at[0]).wait()


def hand_out(count, made, shared, out_hbm, energy_out, energy, sem):
    scales, chan = energy.shape
    stores = [pltpu.make_async_copy(made, out_hbm, sem.at[0])]
    stores[0].start()
    total = jnp.sum(shared[...], axis=0) * (1.0 / count)
    for s in range(scales):
        energy[s : s + 1, :] = total[:, s * chan : (s + 1) * chan]
    stores.append(pltpu.make_async_copy(energy, energy_out, sem.at[1]))
    stores[-1].start(priority=1)
    for store in stores:
        store.wait()


def solution(mesh):
    nx, ny = mesh.shape["gx"], mesh.shape["gy"]
    n = nx * ny

    def shards(
        signals, tiles, tile_dir, tile_mask, live_rows, bound_rows, scale_coeffs, spectral_bound
    ):
        ex, ey, chan, size = signals.shape
        slots = tiles.shape[2]
        scales = scale_coeffs.shape[0]
        nb = ex * ey
        width = -(-scales * chan // 128) * 128
        quads = ey * EDGE // size
        bf, f32 = jnp.bfloat16, jnp.float32
        vmem = pl.BlockSpec(memory_space=pltpu.VMEM)
        hbm = pl.BlockSpec(memory_space=pltpu.HBM)
        rows = [chan + (8 if r == 0 else 0) for r in range(DEG)]
        made, shared = pl.pallas_call(
            functools.partial(kernel, nx, ny),
            out_shape=(
                jax.ShapeDtypeStruct((scales, ex, ey, chan, size), f32),
                jax.ShapeDtypeStruct((n, 1, width), f32),
            ),
            in_specs=[hbm] * 7 + [pl.BlockSpec(memory_space=pltpu.SMEM)],
            out_specs=(vmem, vmem),
            scratch_shapes=[
                pltpu.VMEM(signals.shape, f32),
                pltpu.SMEM((ex, slots, ey), jnp.int32),
                pltpu.SMEM((ex, slots, ey), jnp.int32),
                pltpu.SMEM((ex, ey), jnp.int32),
                pltpu.SMEM((ex, ey), jnp.int32),
                pltpu.SMEM(scale_coeffs.shape, f32),
                pltpu.SMEM((nb * slots,), jnp.int32),
                pltpu.SMEM((nb * slots,), f32),
                pltpu.VMEM((ex, ey, slots, size, size), bf),
                pltpu.VMEM((nb, size, 2 * size), bf),
                [pltpu.VMEM((nb, rows[k], size), bf) for k in range(2)],
                pltpu.VMEM((nb, 2 * rows[0], size), f32),
                pltpu.VMEM((nb, chan, size), f32),
                pltpu.VMEM((DEG + 1, nb, chan, size), f32),
                pltpu.VMEM((nb, 1, size), f32),
                pltpu.VMEM((nb, 1, size), f32),
                [pltpu.VMEM((ZERO + 1, rows[min(k, 1)], size), bf) for k in range(3)],
                [pltpu.VMEM((2, quads, rows[r], size), bf) for r in range(DEG)],
                [pltpu.VMEM((2, quads, rows[r], size), bf) for r in range(DEG)],
                [pltpu.VMEM((2 * ex + 4, rows[r], size), bf) for r in range(DEG)],
                pltpu.SemaphoreType.DMA((1 + GROUPS,)),
                pltpu.SemaphoreType.DMA((1,)),
                pltpu.SemaphoreType.DMA((2, 2)),
                pltpu.SemaphoreType.DMA((1,)),
                pltpu.SemaphoreType.REGULAR((len(STEPS),)),
            ],
            compiler_params=pltpu.CompilerParams(
                collective_id=0, has_side_effects=True, vmem_limit_bytes=VMEM_LIMIT
            ),
        )(
            *[
                pltpu.with_memory_space_constraint(a, pltpu.HBM)
                for a in (
                    signals, tiles, jnp.swapaxes(tile_dir, 1, 2), jnp.swapaxes(tile_mask, 1, 2),
                    live_rows, bound_rows, scale_coeffs,
                )
            ], spectral_bound
        )
        return pl.pallas_call(
            functools.partial(hand_out, n * nb * size),
            out_shape=(
                jax.ShapeDtypeStruct(made.shape, f32),
                jax.ShapeDtypeStruct((scales, chan), f32),
            ),
            in_specs=[vmem] * 2,
            out_specs=(hbm, hbm),
            scratch_shapes=[
                pltpu.VMEM((scales, chan), f32),
                pltpu.SemaphoreType.DMA((2,)),
            ],
            compiler_params=pltpu.CompilerParams(vmem_limit_bytes=VMEM_LIMIT),
        )(made, shared)

    placed = (
        P("gx", "gy", None, None),
        P("gx", "gy", None, None, None),
        P("gx", "gy", None),
        P("gx", "gy", None),
        P("gx", "gy"),
        P("gx", "gy"),
        P(),
        P(),
    )
    return jax.shard_map(
        shards,
        mesh=mesh,
        in_specs=placed,
        out_specs=(P(None, "gx", "gy", None, None), P()),
        check_vma=False,
    )
```
